64 devices in a mesh: dp: 4 (over x, y), sp: 16 (over z, core).
Axes of the slice: x: 2, y: 2, z: 8, core: 2. Of those that a mesh axis runs over, the one named last changes fastest.
The devices are a block of a 4x4x8 slice.
Arguments:
- x: bfloat16 [32768, 2560], P(('dp', 'sp')), parts along dimension 0
- gain: bfloat16 [2560], replicated
- wq: bfloat16 [2560, 2048], P('sp')
- wk: bfloat16 [2560, 1024], P('sp')
- wv: bfloat16 [2560, 1024], P('sp')
- wo: bfloat16 [2048, 2560], P('sp')
Outputs:
- output: bfloat16 [32768, 2560], P(('dp', 'sp')), parts along dimension 0
There are 4 independent parts. The reference program is written for one: setup_inputs(seed, part) draws one part's arguments, and reference() takes and returns one part's arrays. A program takes and returns all parts, laid end to end along the dimension named above; an argument that names none is the same for every part.
All inputs are finite; a program needn't handle non-finite values.
Results may differ from the reference program's by a relative error of at most 0.012.
Values are sent between devices in bfloat16 or wider.
A program may use at most 768 MiB of HBM per device.

```python
import jax
import jax.numpy as jnp
from jax import lax

ROWS = 8192
D = 2560
HEADS = 8
KV_HEADS = 4
HEAD = 256
THETA = 10000


def setup_inputs(seed: int = 0, part: int = 0) -> dict:
    kx, kn, kq, kk, kv, ko = jax.random.split(jax.random.key(seed), 6)

    def weights(key, rows, columns):
        return jax.random.normal(key, (rows, columns), jnp.float32) * rows**-0.5

    drawn = {
        "x": jax.random.normal(jax.random.fold_in(kx, part), (ROWS, D), jnp.float32),
        "gain": 1 + 0.1 * jax.random.normal(kn, (D,), jnp.float32),
        "wq": 2 * weights(kq, D, HEADS * HEAD),
        "wk": 2 * weights(kk, D, KV_HEADS * HEAD),
        "wv": 4 * weights(kv, D, KV_HEADS * HEAD),
        "wo": weights(ko, HEADS * HEAD, D),
    }
    return {k: v.astype(jnp.bfloat16) for k, v in drawn.items()}


def normed(x, gain):
    wide = x.astype(jnp.float32)
    scale = lax.rsqrt(jnp.mean(wide * wide, -1, keepdims=True) + 1e-6)
    return (wide * scale * gain.astype(jnp.float32)).astype(jnp.bfloat16)


def turned(t, place, theta):
    half = t.shape[-1] // 2
    angle = place.astype(jnp.float32)[:, None] * theta ** (-jnp.arange(half, dtype=jnp.float32) / half)
    cos, sin = jnp.cos(angle)[:, None], jnp.sin(angle)[:, None]
    a, b = t[..., :half].astype(jnp.float32), t[..., half:].astype(jnp.float32)
    return jnp.concatenate([a * cos - b * sin, b * cos + a * sin], -1).astype(jnp.bfloat16)


def matmul(a, w):
    return jnp.dot(a, w, preferred_element_type=jnp.float32).astype(jnp.bfloat16)


def einsum(form, a, b):
    return jnp.einsum(form, a.astype(jnp.float32), b.astype(jnp.float32))


def attention(q, k, v):
    scores = einsum("tgsd,ugd->gstu", q, k) * q.shape[-1] ** -0.5
    token = jnp.arange(q.shape[0])
    scores = jnp.where(token[:, None] >= token, scores, -jnp.inf)
    weights = jax.nn.softmax(scores, -1).astype(jnp.bfloat16)
    return einsum("gstu,ugd->tgsd", weights, v).astype(jnp.bfloat16)


def reference(x, gain, wq, wk, wv, wo):
    a, place = normed(x, gain), jnp.arange(ROWS)
    q = turned(matmul(a, wq).reshape(ROWS, HEADS, HEAD), place, THETA).reshape(ROWS, KV_HEADS, -1, HEAD)
    k = turned(matmul(a, wk).reshape(ROWS, KV_HEADS, HEAD), place, THETA)
    v = matmul(a, wv).reshape(ROWS, KV_HEADS, HEAD)
    seen = attention(q, k, v).reshape(ROWS, HEADS * HEAD)
    return (x.astype(jnp.float32) + jnp.dot(seen, wo, preferred_element_type=jnp.float32)).astype(jnp.bfloat16)
```

```python
import functools
import math

import jax
import jax.numpy as jnp
from jax import lax
from jax.experimental import pallas as pl
from jax.experimental.pallas import tpu as pltpu
from jax.sharding import PartitionSpec as P

HEAD = 256
THETA = 10000
NEG = -1e30
HIDDEN = 2 * NEG
LOG2E = 1.4426950408889634
VMEM = 67_000_000
MESH = pl.DeviceIdType.MESH
BK = 512
PLUS, MINUS = 0, 1


def _dot(a, b, ca, cb):
    return lax.dot_general(a, b, (((ca,), (cb,)), ((), ())), preferred_element_type=jnp.float32)


def _turn(t, cos, sin):
    half = t.shape[-1] // 2
    a, b = t[:, :half].astype(jnp.float32), t[:, half:].astype(jnp.float32)
    return jnp.concatenate([a * cos - b * sin, b * cos + a * sin], -1).astype(jnp.bfloat16)


class Ids:
    def __init__(self):
        self.of = {}

    def __call__(self, *key):
        return self.of.setdefault(key, len(self.of))


def _kernel(chips, side, x_ref, gain_ref, cos_ref, sin_ref, wq_ref, wk_ref, wv_ref, wo_ref, y_ref,
            a_s, wkv_s, wq_s, wo_s, k_s, v_s, q_s, top_s, mix_s, send, recv, kv_send, kv_recv, local, out_sem):
    own, width = x_ref.shape
    tokens = 2 * own
    kvh = k_s.shape[1]
    per = q_s.shape[1] // tokens
    far = chips // 2
    g, sp = lax.axis_index("dp"), lax.axis_index("sp")
    z, c = sp // 2, sp % 2
    gx, gy = g // side, g % side
    xb, yb = gx % 2, gy % 2
    gx_n = g + (1 - 2 * xb) * side
    gy_n = g + (1 - 2 * yb)
    gd_n = gx_n + (1 - 2 * yb)
    partner = (g, 2 * z + 1 - c)
    chip_at = lambda dr, d: (z - d + chips) % chips if dr == PLUS else (z + d) % chips
    onward = [(g, 2 * ((z + 1) % chips) + c), (g, 2 * ((z + chips - 1) % chips) + c)]
    beside = {"x": (gx_n, sp), "y": (gy_n, sp), "d": (gd_n, sp)}
    ids = Ids()
    sent, sent_q = [], []

    def copy(key, src, dst, to):
        n = ids(*key)
        return pltpu.make_async_remote_copy(src_ref=src, dst_ref=dst, send_sem=send.at[n], recv_sem=recv.at[n], device_id=to, device_id_type=MESH)

    def start(key, src, dst, to):
        t = copy(key, src, dst, to)
        t.start()
        (sent_q if key[0] in ("q", "qx", "qy", "qd") else sent).append(t)

    def arrived(key, dst):
        copy(key, dst, dst, partner).wait_recv()

    def rows(w, chip, part, parts, half=None):
        deep = w.shape[0] // chips // parts
        cols = slice(None) if half is None else pl.ds(half * (w.shape[1] // 2), w.shape[1] // 2)
        return w.at[pl.ds(pl.multiple_of(chip * (w.shape[0] // chips) + part * deep, 16), deep), cols]

    wo_own = wo_s.at[c]

    def pieces(core):
        hk, hq, ho = wk_ref.shape[1] // 2, wq_ref.shape[1] // 2, wo_ref.shape[1] // 2
        at = lambda ref, n: ref.at[:, pl.ds(pl.multiple_of(core * n, 128), n)]
        kv = rows(wkv_s, z, c, 2)
        return [
            (at(wk_ref, hk), rows(wkv_s, z, c, 2, 0)),
            (at(wv_ref, hk), rows(wkv_s, z, c, 2, 1)),
            (at(wq_ref, hq), rows(wq_s, z, c, 2)),
            (at(wo_ref, ho), rows(wo_s.at[core], z, c, 2)),
        ]

    mine = pieces(c)
    theirs = pieces(1 - c)
    landed = [rows(wkv_s, z, 1 - c, 2, 0), rows(wkv_s, z, 1 - c, 2, 1), rows(wq_s, z, 1 - c, 2), rows(wo_own, z, 1 - c, 2)]
    local_copies = [pltpu.make_async_copy(s, t, local.at[n]) for n, (s, t) in enumerate(mine)]
    for t in local_copies:
        t.start()

    barrier = pltpu.get_barrier_semaphore()
    around = [*onward, *beside.values(), partner]
    for who in around:
        pl.semaphore_signal(barrier, inc=1, device_id=who, device_id_type=MESH)
    pl.semaphore_wait(barrier, len(around))

    for n, (s, t) in enumerate(theirs):
        if n == 2:
            start(("swap", "x"), x_ref, a_s.at[pl.ds(pl.multiple_of(c * own, 16), own), :], partner)
        start(("swap", n), s, t, partner)

    p = (xb + yb) % 2
    first_parts = [2 * p, 2 * p + 1]
    other_parts = [2 * (1 - p), 2 * (1 - p) + 1]
    for n in (0, 1):
        local_copies[n].wait()
    for n in (0, 1):
        arrived(("swap", n), landed[n])
    for i in (0, 1):
        for dr in (PLUS, MINUS):
            r = rows(wkv_s, z, first_parts[i], 4)
            start(("kv", i, dr, 1), r, r, onward[dr])

    arrived(("swap", "x"), a_s.at[pl.ds(pl.multiple_of((1 - c) * own, 16), own), :])
    step = 64
    gain = gain_ref[...].astype(jnp.float32)

    def norm(wide):
        wide = wide.astype(jnp.float32)
        scale = lax.rsqrt(jnp.mean(wide * wide, -1, keepdims=True) + 1e-6)
        return (wide * scale * gain).astype(jnp.bfloat16)

    def norm_rows(i, _):
        here = pl.ds(pl.multiple_of((1 - c) * own + i * step, step), step)
        a_s[here, :] = norm(a_s[here, :])
        there = pl.ds(pl.multiple_of(c * own + i * step, step), step)
        a_s[there, :] = norm(x_ref[pl.ds(pl.multiple_of(i * step, step), step), :])

    lax.fori_loop(0, own // step, norm_rows, None)

    hops = [(i, dr, d) for d in range(1, far) for i in (0, 1) for dr in (PLUS, MINUS)] + [(0, PLUS, far), (1, MINUS, far)]
    for i, dr, d in hops:
        r = rows(wkv_s, chip_at(dr, d), first_parts[i], 4)
        arrived(("kv", i, dr, d), r)
        if d + 1 < far or (d + 1 == far and i == dr):
            start(("kv", i, dr, d + 1), r, r, onward[dr])
        start(("kvn", i, dr, d), r, r, beside["xy"[i]])

    quarter = 2 * xb + yb
    quarters = {"x": 2 * (1 - xb) + yb, "y": 2 * xb + 1 - yb, "d": 2 * (1 - xb) + 1 - yb}
    mats = {"q": wq_s, "o": wo_own}
    for n in (2, 3):
        local_copies[n].wait()
        arrived(("swap", n), landed[n])
    for m, w in mats.items():
        for dr in (PLUS, MINUS):
            r = rows(w, z, quarter, 4)
            start((m, dr, 1), r, r, onward[dr])

    for i, dr, d in hops:
        arrived(("kvn", i, dr, d), rows(wkv_s, chip_at(dr, d), other_parts[i], 4))

    block = 256
    kcols = kvh * HEAD

    def project_kv(b, _):
        at = pl.ds(pl.multiple_of(b * block, block), block)
        r = _dot(a_s[at, :], wkv_s[...], 1, 0).astype(jnp.bfloat16)
        for h in range(kvh):
            k_s[z, h, at, :] = _turn(r[:, h * HEAD : (h + 1) * HEAD], cos_ref[at, :], sin_ref[at, :])
            v_s[z, h, :, at] = r[:, kcols + h * HEAD : kcols + (h + 1) * HEAD].T

    lax.fori_loop(0, tokens // block, project_kv, None)

    hops4 = [(dr, d) for d in range(1, far + 1) for dr in (PLUS, MINUS)]
    half_of = lambda dr, d: None if d < far else dr
    later = []
    for dr, d in hops4:
        for m, w in mats.items():
            r = rows(w, chip_at(dr, d), quarter, 4, half_of(dr, d))
            arrived((m, dr, d), r)
            if d < far:
                f = rows(w, chip_at(dr, d), quarter, 4, half_of(dr, d + 1))
                start((m, dr, d + 1), f, f, onward[dr])
            for way in ("x", "y", "d"):
                args = ((m + way, dr, d), r, r, beside[way])
                if m == "q":
                    start(*args)
                else:
                    later.append(args)
    for args in later:
        start(*args)

    def kv_copy(dr, d, h, part, j, to):
        n = ((dr * far + d - 1) * kvh + h) * 2 + part
        ref = (k_s if part == 0 else v_s).at[j, h]
        return pltpu.make_async_remote_copy(src_ref=ref, dst_ref=ref, send_sem=kv_send.at[n], recv_sem=kv_recv.at[n], device_id=to,
                                            device_id_type=MESH)

    def made(dr, d, h, at):
        mid = kvh // 2
        up = h < mid
        reach = far - jnp.where(dr == PLUS, jnp.where(up, 0, 1), jnp.where(up, 1, 0))
        j = jnp.where(dr == PLUS, at - d, at + d)
        j = jnp.where(j >= chips, j - chips, j)
        ok = (d >= 1) & (d <= reach) & jnp.where(dr == PLUS, j >= 0, j < reach)
        return ok, jnp.where(j < 0, 0, j)

    for h in range(kvh):
        for part in (0, 1):
            for dr in (PLUS, MINUS):
                go, _ = made(dr, 1, h, z + 1 if dr == PLUS else (z + chips - 1) % chips)
                if dr == PLUS:
                    go &= z + 1 < chips

                @pl.when(go)
                def _():
                    kv_copy(dr, 1, h, part, z, onward[dr]).start()

    for dr, d in hops4:
        for way in ("x", "y", "d"):
            arrived(("q" + way, dr, d), rows(wq_s, chip_at(dr, d), quarters[way], 4, half_of(dr, d)))

    def project_q(b, _):
        at = pl.ds(pl.multiple_of(b * block, block), block)
        r = _dot(a_s[at, :], wq_s[...], 1, 0).astype(jnp.bfloat16)
        for h in range(kvh):
            for n in range(per):
                col = (h * per + n) * HEAD
                q_s[h, pl.ds(pl.multiple_of(n * tokens + b * block, block), block), :] = _turn(r[:, col : col + HEAD], cos_ref[at, :], sin_ref[at, :])

    lax.fori_loop(0, tokens // block, project_q, None)

    e = HEAD**-0.5 * LOG2E
    strips = list(range(0, per * tokens, BK))
    ones = jnp.ones((8, BK), jnp.bfloat16)

    def attend(j, h, b, chosen):
        here = pl.ds(pl.multiple_of(b * BK, BK), BK)
        keys = k_s[j, h, here, :]
        values = jnp.concatenate([v_s[j, h, :, here], ones], axis=0)
        scores = [_dot(keys, q_s[h, at : at + BK, :], 1, 1) for at, _ in chosen]
        weights, keeps = [], []
        for (at, cut), s in zip(chosen, scores):
            if cut:
                s = jnp.where(lax.broadcasted_iota(jnp.int32, s.shape, 1) >= lax.broadcasted_iota(jnp.int32, s.shape, 0), s, HIDDEN)
            old = top_s[h, :, at : at + BK]
            top = jnp.maximum(old, s.max(axis=0, keepdims=True))
            top_s[h, :, at : at + BK] = top
            weights.append(jnp.exp2((s - top) * e).astype(jnp.bfloat16))
            keeps.append(jnp.exp2((old - top) * e))
        for (at, _), w, keep in zip(chosen, weights, keeps):
            mix_s[h, :, at : at + BK] = mix_s[h, :, at : at + BK] * keep + _dot(values, w, 1, 0)

    def own_keys(h, _):
        top_s[h] = jnp.full(top_s.shape[1:], NEG, jnp.float32)
        mix_s[h] = jnp.zeros(mix_s.shape[1:], jnp.float32)
        for b in range(tokens // BK):
            attend(z, h, b, [(at, at % tokens == b * BK) for at in strips if at % tokens >= b * BK])

    lax.fori_loop(0, kvh, own_keys, None)

    wo_copy = copy(("wo",), wo_own, wo_own, partner)
    sent.append(wo_copy)

    def hop(i, _):
        d, h, dr = i // (2 * kvh) + 1, (i // 2) % kvh, i % 2

        @pl.when(i == 2 * (2 * kvh))
        def _():
            for dr_, d_ in hops4:
                for way in ("x", "y", "d"):
                    arrived(("o" + way, dr_, d_), rows(wo_own, chip_at(dr_, d_), quarters[way], 4, half_of(dr_, d_)))
            for t in sent_q:
                t.wait_send()
            wo_copy.start()

        here, j = made(dr, d, h, z)

        @pl.when(here)
        def _():
            nxt = jnp.where(dr == PLUS, z + 1, (z + chips - 1) % chips)
            on, _ = made(dr, d + 1, h, nxt)
            on &= nxt < chips
            for part in (0, 1):
                kv_copy(dr, d, h, part, j, partner).wait_recv()

                @pl.when(on)
                def _():
                    kv_copy(dr, d + 1, h, part, j, (g, 2 * (nxt % chips) + c)).start()

            @pl.when(j < z)
            def _():
                def one(b, _):
                    attend(j, h, b, [(at, False) for at in strips])

                lax.fori_loop(0, tokens // BK, one, None)

    lax.fori_loop(0, far * 2 * kvh, hop, None)

    arrived(("wo",), wo_s.at[1 - c])
    seen = lambda core: wq_s.at[pl.ds(pl.multiple_of(core * own, 16), own), :]
    stage = wq_s.at[pl.ds(2 * own, own), :]

    def finish(ref, core):
        for h in range(kvh):
            for n in range(per):
                at = pl.ds(pl.multiple_of(n * tokens + core * own, own), own)
                out = mix_s[h, :HEAD, at] * (1 / mix_s[h, HEAD : HEAD + 1, at])
                col = (h * per + n) * HEAD
                ref[:, col : col + HEAD] = out.T.astype(jnp.bfloat16)

    finish(stage, 1 - c)
    finish(seen(c), c)
    start(("seen",), stage, seen(c), partner)
    arrived(("seen",), seen(1 - c))

    half = wo_s.shape[2]
    cols = 256
    many = half // cols

    def out_copy(i):
        at = pl.ds(pl.multiple_of(i * cols, cols), cols)
        return pltpu.make_async_copy(a_s.at[pl.ds(0, own), at], y_ref.at[:, at], out_sem.at[i])

    def project_out(i, _):
        core, n = i // many, i % many
        at = pl.ds(pl.multiple_of(n * cols, cols), cols)
        to = pl.ds(pl.multiple_of(i * cols, cols), cols)
        deep = wo_s.shape[1] // 2
        y = _dot(wq_s[:own, :], wo_s[core, :deep, at], 1, 0) + _dot(wq_s[own : 2 * own, :], wo_s[core, deep:, at], 1, 0)
        a_s[:own, to] = (x_ref[:, to].astype(jnp.float32) + y).astype(jnp.bfloat16)
        out_copy(i).start()

    lax.fori_loop(0, 2 * many, project_out, None)
    lax.fori_loop(0, 2 * many, lambda i, _: out_copy(i).wait(), None)

    for t in sent:
        t.wait_send()

    def left(i, _):
        d, h, dr = i // (2 * kvh) + 1, (i // 2) % kvh, i % 2
        nxt = jnp.where(dr == PLUS, z + 1, (z + chips - 1) % chips)
        on, j = made(dr, d, h, nxt)

        @pl.when(on & (nxt < chips))
        def _():
            for part in (0, 1):
                kv_copy(dr, d, h, part, j, partner).wait_send()

    lax.fori_loop(0, far * 2 * kvh, left, None)


def _transfers(far):
    first = 4 * (far - 1) + 2
    other = 2 * far
    return 5 + 2 * first + 2 * 4 * other + 2


def solution(mesh):
    chips = mesh.shape["sp"] // 2
    side = math.isqrt(mesh.shape["dp"])

    def step(x, gain, wq, wk, wv, wo):
        own, width = x.shape
        tokens = 2 * own
        z = lax.axis_index("sp") // 2
        half = HEAD // 2
        place = z * tokens + jnp.arange(tokens)
        angle = place.astype(jnp.float32)[:, None] * THETA ** (-jnp.arange(half, dtype=jnp.float32) / half)
        cos, sin = jnp.cos(angle), jnp.sin(angle)
        kvh = wk.shape[1] // HEAD // 2
        per = wq.shape[1] // wk.shape[1]
        far = chips // 2
        vm, hbm = pl.BlockSpec(memory_space=pltpu.VMEM), pl.BlockSpec(memory_space=pl.ANY)
        deep = wo.shape[0] * 2 * chips
        many = _transfers(far)
        return pl.pallas_call(
            functools.partial(_kernel, chips, side),
            out_shape=jax.ShapeDtypeStruct((own, width), jnp.bfloat16),
            in_specs=[vm] * 4 + [hbm] * 4,
            out_specs=hbm,
            scratch_shapes=[
                pltpu.VMEM((tokens, width), jnp.bfloat16),
                pltpu.VMEM((width, wk.shape[1]), jnp.bfloat16),
                pltpu.VMEM((width, wq.shape[1] // 2), jnp.bfloat16),
                pltpu.VMEM((2, deep, width // 2), jnp.bfloat16),
                pltpu.VMEM((chips, kvh, tokens, HEAD), jnp.bfloat16),
                pltpu.VMEM((chips, kvh, HEAD, tokens), jnp.bfloat16),
                pltpu.VMEM((kvh, per * tokens, HEAD), jnp.bfloat16),
                pltpu.VMEM((kvh, 1, per * tokens), jnp.float32),
                pltpu.VMEM((kvh, HEAD + 8, per * tokens), jnp.float32),
                pltpu.SemaphoreType.DMA((many,)),
                pltpu.SemaphoreType.DMA((many,)),
                pltpu.SemaphoreType.DMA((2 * far * kvh * 2,)),
                pltpu.SemaphoreType.DMA((2 * far * kvh * 2,)),
                pltpu.SemaphoreType.DMA((4,)),
                pltpu.SemaphoreType.DMA((width // 256,)),
            ],
            compiler_params=pltpu.CompilerParams(collective_id=0, has_side_effects=True, vmem_limit_bytes=VMEM),
            name="layer",
        )(x, gain.reshape(1, -1), cos, sin, wq, wk, wv, wo)

    tokens, whole = P(("dp", "sp"), None), P("sp", None)
    return jax.shard_map(
        step,
        mesh=mesh,
        in_specs=(tokens, P(None), whole, whole, whole, whole),
        out_specs=tokens,
        check_vma=False,
    )
```

```python
import functools
import math

import jax
import jax.numpy as jnp
import numpy as np
from jax import lax
from jax.experimental import pallas as pl
from jax.experimental.pallas import tpu as pltpu
from jax.sharding import PartitionSpec as P

HEAD = 256
THETA = 10000
NEG = -1e30
HIDDEN = 2 * NEG
LOG2E = 1.4426950408889634
VMEM = 67_000_000
MESH = pl.DeviceIdType.MESH
BK = 512
PLUS, MINUS = 0, 1


def _dot(a, b, ca, cb):
    return lax.dot_general(a, b, (((ca,), (cb,)), ((), ())), preferred_element_type=jnp.float32)


def _turn(t, cos, sin):
    half = t.shape[-1] // 2
    a, b = t[:, :half].astype(jnp.float32), t[:, half:].astype(jnp.float32)
    return jnp.concatenate([a * cos - b * sin, b * cos + a * sin], -1).astype(jnp.bfloat16)


class Ids:
    def __init__(self):
        self.of = {}

    def __call__(self, *key):
        return self.of.setdefault(key, len(self.of))


def _kernel(chips, side, x_ref, gain_ref, freq_ref, wq_ref, wk_ref, wv_ref, wo_ref, y_ref,
            a_s, wk_s, wv_s, wq_s, wo_s, k_s, v_s, q_s, top_s, mix_s, cos_s, sin_s, sum_s, send, recv, kv_send, kv_recv, local, out_sem):
    own, width = x_ref.shape
    tokens = 2 * own
    kvh = k_s.shape[1]
    per = q_s.shape[1] // tokens
    far = chips // 2
    g, sp = lax.axis_index("dp"), lax.axis_index("sp")
    z, c = sp // 2, sp % 2
    gx, gy = g // side, g % side
    xb, yb = gx % 2, gy % 2
    gx_n = g + (1 - 2 * xb) * side
    gy_n = g + (1 - 2 * yb)
    gd_n = gx_n + (1 - 2 * yb)
    partner = (g, 2 * z + 1 - c)
    chip_at = lambda dr, d: (z - d + chips) % chips if dr == PLUS else (z + d) % chips
    onward = [(g, 2 * ((z + 1) % chips) + c), (g, 2 * ((z + chips - 1) % chips) + c)]
    beside = {"x": (gx_n, sp), "y": (gy_n, sp), "d": (gd_n, sp)}
    ids = Ids()
    sent, sent_q = [], []

    def copy(key, src, dst, to):
        n = ids(*key)
        return pltpu.make_async_remote_copy(src_ref=src, dst_ref=dst, send_sem=send.at[n], recv_sem=recv.at[n], device_id=to, device_id_type=MESH)

    def start(key, src, dst, to):
        t = copy(key, src, dst, to)
        t.start()
        (sent_q if key[0] in ("q", "qx", "qy", "qd") else sent).append(t)

    def arrived(key, dst):
        copy(key, dst, dst, partner).wait_recv()

    def rows(w, chip, part, parts, half=None):
        deep = w.shape[0] // chips // parts
        cols = slice(None) if half is None else pl.ds(half * (w.shape[1] // 2), w.shape[1] // 2)
        return w.at[pl.ds(pl.multiple_of(chip * (w.shape[0] // chips) + part * deep, 16), deep), cols]

    wo_own = wo_s.at[c]

    mats = {"k": wk_s, "v": wv_s, "q": wq_s, "o": wo_own}
    given = {"k": wk_ref, "v": wv_ref, "q": wq_ref, "o": wo_ref}

    def piece(m, core):
        n = given[m].shape[1] // 2
        return given[m].at[:, pl.ds(pl.multiple_of(core * n, 128), n)]

    local_copies = {m: pltpu.make_async_copy(piece(m, c), rows(w, z, c, 2), local.at[n]) for n, (m, w) in enumerate(mats.items())}
    for t in local_copies.values():
        t.start()

    barrier = pltpu.get_barrier_semaphore()
    around = [*onward, *beside.values(), partner]
    for who in around:
        pl.semaphore_signal(barrier, inc=1, device_id=who, device_id_type=MESH)
    pl.semaphore_wait(barrier, len(around))

    for m in mats:
        target = wo_s.at[1 - c] if m == "o" else mats[m]
        start(("swap", m), piece(m, 1 - c), rows(target, z, c, 2), partner)
        if m == "v":
            start(("swap", "x"), x_ref, a_s.at[pl.ds(pl.multiple_of(c * own, 16), own), :], partner)

    quarter = 2 * xb + yb
    quarters = {"x": 2 * (1 - xb) + yb, "y": 2 * xb + 1 - yb, "d": 2 * (1 - xb) + 1 - yb}
    half_of = lambda dr, d: None if d < far else dr
    hops = [(dr, d) for d in range(1, far + 1) for dr in (PLUS, MINUS)]

    def set_off(names):
        for m in names:
            local_copies[m].wait()
            arrived(("swap", m), rows(mats[m], z, 1 - c, 2))
        for m in names:
            for dr in (PLUS, MINUS):
                r = rows(mats[m], z, quarter, 4)
                start((m, dr, 1), r, r, onward[dr])

    def pass_on(names, d):
        for dr in (PLUS, MINUS):
            for m in names:
                r = rows(mats[m], chip_at(dr, d), quarter, 4, half_of(dr, d))
                arrived((m, dr, d), r)
                if d < far:
                    f = rows(mats[m], chip_at(dr, d), quarter, 4, half_of(dr, d + 1))
                    start((m, dr, d + 1), f, f, onward[dr])

    def share(m, ds):
        for d in ds:
            for dr in (PLUS, MINUS):
                r = rows(mats[m], chip_at(dr, d), quarter, 4, half_of(dr, d))
                for way in ("x", "y", "d"):
                    start((m + way, dr, d), r, r, beside[way])

    def shared(m):
        for dr, d in hops:
            for way in ("x", "y", "d"):
                arrived((m + way, dr, d), rows(mats[m], chip_at(dr, d), quarters[way], 4, half_of(dr, d)))

    set_off("kv")

    arrived(("swap", "x"), a_s.at[pl.ds(pl.multiple_of((1 - c) * own, 16), own), :])
    step = 64
    gain = gain_ref[...].astype(jnp.float32).reshape(1, -1)

    def norm(wide):
        wide = wide.astype(jnp.float32)
        scale = lax.rsqrt(jnp.mean(wide * wide, -1, keepdims=True) + 1e-6)
        return (wide * scale * gain).astype(jnp.bfloat16)

    def norm_rows(i, _):
        here = pl.ds(pl.multiple_of((1 - c) * own + i * step, step), step)
        a_s[here, :] = norm(a_s[here, :])
        there = pl.ds(pl.multiple_of(c * own + i * step, step), step)
        a_s[there, :] = norm(x_ref[pl.ds(pl.multiple_of(i * step, step), step), :])

    lax.fori_loop(0, own // step, norm_rows, None)

    place = (z * tokens + lax.broadcasted_iota(jnp.int32, (own, 1), 0)).astype(jnp.float32)
    for i in range(2):
        angle = (place + i * own) * freq_ref[...]
        cos_s[i * own : (i + 1) * own, :] = jnp.cos(angle)
        sin_s[i * own : (i + 1) * own, :] = jnp.sin(angle)

    for d in range(1, far + 1):
        pass_on("kv", d)
        share("k", [d])
        if d == 1:
            set_off("qo")
        if d > 2:
            pass_on("qo", d - 2)
    share("v", range(1, far + 1))
    pass_on("qo", far - 1)

    block = 256

    def project_k(b, _):
        at = pl.ds(pl.multiple_of(b * block, block), block)
        r = _dot(a_s[at, :], wk_s[...], 1, 0).astype(jnp.bfloat16)
        for h in range(kvh):
            k_s[z, h, at, :] = _turn(r[:, h * HEAD : (h + 1) * HEAD], cos_s[at, :], sin_s[at, :])

    def project_v(b, _):
        at = pl.ds(pl.multiple_of(b * block, block), block)
        r = _dot(a_s[at, :], wv_s[...], 1, 0).astype(jnp.bfloat16)
        for h in range(kvh):
            v_s[z, h, :, at] = r[:, h * HEAD : (h + 1) * HEAD].T

    nb = tokens // BK

    def kv_copy(dr, d, h, b, part, j, to):
        n = (((dr * far + d - 1) * kvh + h) * nb + b) * 2 + part
        here = pl.ds(pl.multiple_of(b * BK, BK), BK)
        ref = v_s.at[j, h, :, here] if part else k_s.at[j, h, here, :]
        return pltpu.make_async_remote_copy(src_ref=ref, dst_ref=ref, send_sem=kv_send.at[n], recv_sem=kv_recv.at[n], device_id=to,
                                            device_id_type=MESH)

    def made(dr, d, h, at):
        mid = kvh // 2
        up = h < mid
        reach = far - jnp.where(dr == PLUS, jnp.where(up, 0, 1), jnp.where(up, 1, 0))
        j = jnp.where(dr == PLUS, at - d, at + d)
        j = jnp.where(j >= chips, j - chips, j)
        ok = (d >= 1) & (d <= reach) & jnp.where(dr == PLUS, j >= 0, j < reach)
        return ok, jnp.where(j < 0, 0, j)

    def begin(part):
        for h in range(kvh):
            for dr in (PLUS, MINUS):
                go, _ = made(dr, 1, h, z + 1 if dr == PLUS else (z + chips - 1) % chips)
                if dr == PLUS:
                    go &= z + 1 < chips

                @pl.when(go)
                def _():
                    for b in range(nb):
                        kv_copy(dr, 1, h, b, part, z, onward[dr]).start()

    def relay(dr, d, h, b, parts):
        here, j = made(dr, d, h, z)
        nxt = jnp.where(dr == PLUS, z + 1, (z + chips - 1) % chips)
        on, _ = made(dr, d + 1, h, nxt)
        for part in parts:

            @pl.when(here)
            def _():
                kv_copy(dr, d, h, b, part, j, partner).wait_recv()

                @pl.when(on & (nxt < chips))
                def _():
                    kv_copy(dr, d + 1, h, b, part, j, (g, 2 * (nxt % chips) + c)).start()

    shared("k")
    lax.fori_loop(0, tokens // block, project_k, None)
    begin(0)
    pass_on("qo", far)
    share("q", range(1, far + 1))
    share("o", range(1, far + 1))
    shared("v")
    lax.fori_loop(0, tokens // block, project_v, None)
    begin(1)

    def first_hop(i, _):
        part, h, b, dr = i // (2 * nb * kvh), (i // (2 * nb)) % kvh, (i // 2) % nb, i % 2
        n_parts = 2
        for q in range(n_parts):

            @pl.when(part == q)
            def _():
                relay(dr, 1, h, b, [q])

    lax.fori_loop(0, 2 * kvh * nb * 2, first_hop, None)

    shared("q")

    def project_q(b, _):
        at = pl.ds(pl.multiple_of(b * block, block), block)
        r = _dot(a_s[at, :], wq_s[...], 1, 0).astype(jnp.bfloat16)
        for h in range(kvh):
            for n in range(per):
                col = (h * per + n) * HEAD
                q_s[h, pl.ds(pl.multiple_of(n * tokens + b * block, block), block), :] = _turn(r[:, col : col + HEAD], cos_s[at, :], sin_s[at, :])

    lax.fori_loop(0, tokens // block, project_q, None)

    e = HEAD**-0.5 * LOG2E
    strips = list(range(0, per * tokens, BK))
    ones = jnp.ones((8, BK), jnp.bfloat16)

    def attend(j, h, b, chosen):
        here = pl.ds(pl.multiple_of(b * BK, BK), BK)
        keys = k_s[j, h, here, :]
        values = jnp.concatenate([v_s[j, h, :, here], ones], axis=0)
        scores = [_dot(keys, q_s[h, at : at + BK, :], 1, 1) for at, _ in chosen]
        weights, keeps = [], []
        for (at, cut), s in zip(chosen, scores):
            if cut:
                s = jnp.where(lax.broadcasted_iota(jnp.int32, s.shape, 1) >= lax.broadcasted_iota(jnp.int32, s.shape, 0), s, HIDDEN)
            old = top_s[h, :, at : at + BK]
            top = jnp.maximum(old, s.max(axis=0, keepdims=True))
            top_s[h, :, at : at + BK] = top
            weights.append(jnp.exp2((s - top) * e).astype(jnp.bfloat16))
            keeps.append(jnp.exp2((old - top) * e))
        for (at, _), w, keep in zip(chosen, weights, keeps):
            mix_s[h, :, at : at + BK] = mix_s[h, :, at : at + BK] * keep + _dot(values, w, 1, 0)

    def own_keys(h, _):
        top_s[h] = jnp.full(top_s.shape[1:], NEG, jnp.float32)
        mix_s[h] = jnp.zeros(mix_s.shape[1:], jnp.float32)
        for b in range(tokens // BK):
            attend(z, h, b, [(at, at % tokens == b * BK) for at in strips if at % tokens >= b * BK])

    lax.fori_loop(0, kvh, own_keys, None)

    wo_copy = copy(("wo",), wo_own, wo_own, partner)
    sent.append(wo_copy)

    def hop(i, _):
        d, h, dr = i // (2 * kvh) + 1, (i // 2) % kvh, i % 2

        @pl.when(i == 2 * (2 * kvh))
        def _():
            shared("o")
            for t in sent_q:
                t.wait_send()
            wo_copy.start()

        here, j = made(dr, d, h, z)

        @pl.when(here)
        def _():
            def one(b, _):
                @pl.when(d > 1)
                def _():
                    relay(dr, d, h, b, [0, 1])

                @pl.when(j < z)
                def _():
                    attend(j, h, b, [(at, False) for at in strips])

            lax.fori_loop(0, nb, one, None)

    lax.fori_loop(0, far * 2 * kvh, hop, None)

    arrived(("wo",), wo_s.at[1 - c])
    seen = lambda core: wq_s.at[pl.ds(pl.multiple_of(core * own, 16), own), :]
    stage = wq_s.at[pl.ds(2 * own, own), :]

    def finish(ref, core, h):
        for n in range(per):
            at = pl.ds(pl.multiple_of(n * tokens + core * own, own), own)
            out = mix_s[h, :HEAD, at] * (1 / mix_s[h, HEAD : HEAD + 1, at])
            col = (h * per + n) * HEAD
            ref[:, col : col + HEAD] = out.T.astype(jnp.bfloat16)

    for h in range(kvh):
        finish(stage, 1 - c, h)
    for h in range(kvh):
        finish(seen(c), c, h)
        if h == 0:
            start(("seen",), stage, seen(c), partner)

    half = wo_s.shape[2]
    cols = 256
    many = half // cols

    def out_copy(i):
        at = pl.ds(pl.multiple_of(i * cols, cols), cols)
        return pltpu.make_async_copy(a_s.at[pl.ds(0, own), at], y_ref.at[:, at], out_sem.at[i])

    deep = wo_s.shape[1] // 2

    def weights_out(i, core):
        return wo_s[i // many, pl.ds(pl.multiple_of(core * deep, deep), deep), pl.ds(pl.multiple_of(i % many * cols, cols), cols)]

    def own_heads(i, _):
        to = pl.ds(pl.multiple_of(i * cols, cols), cols)
        sum_s[:, to] = x_ref[:, to].astype(jnp.float32) + _dot(seen(c)[...], weights_out(i, c), 1, 0)

    lax.fori_loop(0, 2 * many, own_heads, None)
    arrived(("seen",), seen(1 - c))

    def other_heads(i, _):
        to = pl.ds(pl.multiple_of(i * cols, cols), cols)
        a_s[:own, to] = (sum_s[:, to] + _dot(seen(1 - c)[...], weights_out(i, 1 - c), 1, 0)).astype(jnp.bfloat16)
        out_copy(i).start()

    lax.fori_loop(0, 2 * many, other_heads, None)
    lax.fori_loop(0, 2 * many, lambda i, _: out_copy(i).wait(), None)

    for t in sent:
        t.wait_send()

    def left(i, _):
        d, h, dr = i // (2 * kvh) + 1, (i // 2) % kvh, i % 2
        nxt = jnp.where(dr == PLUS, z + 1, (z + chips - 1) % chips)
        on, j = made(dr, d, h, nxt)

        @pl.when(on & (nxt < chips))
        def _():
            for b in range(nb):
                for part in (0, 1):
                    kv_copy(dr, d, h, b, part, j, partner).wait_send()

    lax.fori_loop(0, far * 2 * kvh, left, None)


def _transfers(far):
    return 5 + 4 * 4 * 2 * far + 2


def solution(mesh):
    chips = mesh.shape["sp"] // 2
    side = math.isqrt(mesh.shape["dp"])

    def step(x, gain, wq, wk, wv, wo):
        own, width = x.shape
        tokens = 2 * own
        half = HEAD // 2
        freq = jnp.asarray(THETA ** (-np.arange(half, dtype=np.float32) / half), jnp.float32).reshape(1, half)
        kvh = wk.shape[1] // HEAD // 2
        per = wq.shape[1] // wk.shape[1]
        far = chips // 2
        vm, hbm = pl.BlockSpec(memory_space=pltpu.VMEM), pl.BlockSpec(memory_space=pl.ANY)
        deep = wo.shape[0] * 2 * chips
        many = _transfers(far)
        return pl.pallas_call(
            functools.partial(_kernel, chips, side),
            out_shape=jax.ShapeDtypeStruct((own, width), jnp.bfloat16),
            in_specs=[vm] * 3 + [hbm] * 4,
            out_specs=hbm,
            scratch_shapes=[
                pltpu.VMEM((tokens, width), jnp.bfloat16),
                pltpu.VMEM((width, wk.shape[1] // 2), jnp.bfloat16),
                pltpu.VMEM((width, wv.shape[1] // 2), jnp.bfloat16),
                pltpu.VMEM((width, wq.shape[1] // 2), jnp.bfloat16),
                pltpu.VMEM((2, deep, width // 2), jnp.bfloat16),
                pltpu.VMEM((chips, kvh, tokens, HEAD), jnp.bfloat16),
                pltpu.VMEM((chips, kvh, HEAD, tokens), jnp.bfloat16),
                pltpu.VMEM((kvh, per * tokens, HEAD), jnp.bfloat16),
                pltpu.VMEM((kvh, 1, per * tokens), jnp.float32),
                pltpu.VMEM((kvh, HEAD + 8, per * tokens), jnp.float32),
                pltpu.VMEM((tokens, half), jnp.float32),
                pltpu.VMEM((tokens, half), jnp.float32),
                pltpu.VMEM((own, width), jnp.float32),
                pltpu.SemaphoreType.DMA((many,)),
                pltpu.SemaphoreType.DMA((many,)),
                pltpu.SemaphoreType.DMA((2 * far * kvh * tokens // BK * 2,)),
                pltpu.SemaphoreType.DMA((2 * far * kvh * tokens // BK * 2,)),
                pltpu.SemaphoreType.DMA((4,)),
                pltpu.SemaphoreType.DMA((width // 256,)),
            ],
            compiler_params=pltpu.CompilerParams(collective_id=0, has_side_effects=True, vmem_limit_bytes=VMEM),
            name="layer",
        )(x, gain, freq, wq, wk, wv, wo)

    tokens, whole = P(("dp", "sp"), None), P("sp", None)
    return jax.shard_map(
        step,
        mesh=mesh,
        in_specs=(tokens, P(None), whole, whole, whole, whole),
        out_specs=tokens,
        check_vma=False,
    )
```

```python
import functools
import math

import jax
import jax.numpy as jnp
import numpy as np
from jax import lax
from jax.experimental import pallas as pl
from jax.experimental.pallas import tpu as pltpu
from jax.sharding import PartitionSpec as P

HEAD = 256
THETA = 10000
NEG = -1e30
HIDDEN = 2 * NEG
LOG2E = 1.4426950408889634
VMEM = 67_000_000
MESH = pl.DeviceIdType.MESH
BK = 512
PLUS, MINUS = 0, 1


def _dot(a, b, ca, cb):
    return lax.dot_general(a, b, (((ca,), (cb,)), ((), ())), preferred_element_type=jnp.float32)


def _turn(t, cos, sin):
    half = t.shape[-1] // 2
    a, b = t[:, :half].astype(jnp.float32), t[:, half:].astype(jnp.float32)
    return jnp.concatenate([a * cos - b * sin, b * cos + a * sin], -1).astype(jnp.bfloat16)


class Ids:
    def __init__(self):
        self.of = {}

    def __call__(self, *key):
        return self.of.setdefault(key, len(self.of))


def _kernel(chips, side, x_ref, gain_ref, freq_ref, wq_ref, wk_ref, wv_ref, wo_ref, y_ref,
            a_s, wk_s, wv_s, wqa_s, wqb_s, wo_s, k_s, v_s, q_s, top_s, mix_s, cos_s, sin_s, sum_s, send, recv, kv_send, kv_recv, local, out_sem):
    own, width = x_ref.shape
    tokens = 2 * own
    kvh = k_s.shape[1]
    per = q_s.shape[1] // tokens
    far = chips // 2
    g, sp = lax.axis_index("dp"), lax.axis_index("sp")
    z, c = sp // 2, sp % 2
    gx, gy = g // side, g % side
    xb, yb = gx % 2, gy % 2
    gx_n = g + (1 - 2 * xb) * side
    gy_n = g + (1 - 2 * yb)
    partner = (g, 2 * z + 1 - c)
    chip_at = lambda dr, d: (z - d + chips) % chips if dr == PLUS else (z + d) % chips
    onward = [(g, 2 * ((z + 1) % chips) + c), (g, 2 * ((z + chips - 1) % chips) + c)]
    beside = {"x": (gx_n, sp), "y": (gy_n, sp)}
    sent_by, came_by = Ids(), Ids()
    sent = []

    def copy(key, src, dst, to):
        name = key[0]
        of_matrix = len(name) < 3 and name[0] in "kvabo"
        s = sent_by(name[0]) if of_matrix else sent_by(*key)
        r = came_by(name) if name[1:] == "d" else came_by(*key)
        return pltpu.make_async_remote_copy(src_ref=src, dst_ref=dst, send_sem=send.at[s], recv_sem=recv.at[r], device_id=to, device_id_type=MESH)

    def start(key, src, dst, to):
        t = copy(key, src, dst, to)
        t.start()
        if len(key[0]) > 2:
            sent.append(t)

    def arrived(key, dst):
        copy(key, dst, dst, partner).wait_recv()

    def rows(w, chip, part, parts, half=None):
        deep = w.shape[0] // chips // parts
        cols = slice(None) if half is None else pl.ds(half * (w.shape[1] // 2), w.shape[1] // 2)
        return w.at[pl.ds(pl.multiple_of(chip * (w.shape[0] // chips) + part * deep, 16), deep), cols]

    wo_own = wo_s.at[c]

    mats = {"k": wk_s, "v": wv_s, "a": wqa_s, "b": wqb_s, "o": wo_own}
    given = {"k": wk_ref, "v": wv_ref, "a": wq_ref, "b": wq_ref, "o": wo_ref}

    def piece(m, core):
        n = mats[m].shape[1]
        first = core * (given[m].shape[1] // 2) + (n if m == "b" else 0)
        return given[m].at[:, pl.ds(pl.multiple_of(first, 128), n)]

    local_copies = {m: pltpu.make_async_copy(piece(m, c), rows(w, z, c, 2), local.at[n]) for n, (m, w) in enumerate(mats.items())}
    mine = pl.ds(pl.multiple_of(c * own, 16), own)
    x_copy = pltpu.make_async_copy(x_ref, a_s.at[mine, :], local.at[len(mats)])
    for t in [*local_copies.values(), x_copy]:
        t.start()

    barrier = pltpu.get_barrier_semaphore()
    around = [*onward, *beside.values(), partner]
    for who in around:
        pl.semaphore_signal(barrier, inc=1, device_id=who, device_id_type=MESH)
    pl.semaphore_wait(barrier, len(around))

    for m in mats:
        target = wo_s.at[1 - c] if m == "o" else mats[m]
        start(("swap", m), piece(m, 1 - c), rows(target, z, c, 2), partner)
        if m == "v":
            start(("swap", "x"), x_ref, a_s.at[mine, :], partner)

    quarter = 2 * xb + yb
    quarters = {"x": 2 * (1 - xb) + yb, "y": 2 * xb + 1 - yb, "d": 2 * (1 - xb) + 1 - yb}
    half_of = lambda dr, d: None if d < far else dr
    hops = [(dr, d) for d in range(1, far + 1) for dr in (PLUS, MINUS)]

    def set_off(names):
        for m in names:
            local_copies[m].wait()
            arrived(("swap", m), rows(mats[m], z, 1 - c, 2))
        for m in names:
            for dr in (PLUS, MINUS):
                r = rows(mats[m], z, quarter, 4)
                start((m, dr, 1), r, r, onward[dr])

    def pass_on(names, d):
        for dr in (PLUS, MINUS):
            for m in names:
                r = rows(mats[m], chip_at(dr, d), quarter, 4, half_of(dr, d))
                arrived((m, dr, d), r)
                if d < far:
                    f = rows(mats[m], chip_at(dr, d), quarter, 4, half_of(dr, d + 1))
                    start((m, dr, d + 1), f, f, onward[dr])

    everywhere = range(1, far + 1)

    def share(m, ds=everywhere):
        for d in ds:
            for dr in (PLUS, MINUS):
                r = rows(mats[m], chip_at(dr, d), quarter, 4, half_of(dr, d))
                for way in ("x", "y"):
                    start((m + way, dr, d), r, r, beside[way])

    def across(m, d, dr):
        for side_, way, to in ((PLUS, "x", "y"), (MINUS, "y", "x")):
            if d < far or dr == side_:
                yield side_, way, to

    def pass_across(m, ds=everywhere):
        for d in ds:
            for dr in (PLUS, MINUS):
                for way in ("x", "y"):
                    arrived((m + way, dr, d), rows(mats[m], chip_at(dr, d), quarters[way], 4, half_of(dr, d)))
                for side_, way, to in across(m, d, dr):
                    r = rows(mats[m], chip_at(dr, d), quarters[way], 4, side_)
                    start((m + "d", dr, d, side_), r, r, beside[to])

    def top_of(m, n):
        return mats[m].at[pl.ds(0, mats[m].shape[0] // (4 * chips) * n), :]

    pieces = 2 * far - 1

    def complete(m):
        arrived((m + "d",), top_of(m, pieces))

    def gone(m):
        t = top_of(m, 4 * pieces)
        copy((m, PLUS, 1), t, t, partner).wait_send()

    set_off("kv")

    step = 64

    def norm_rows(i, _):
        here = pl.ds(pl.multiple_of(i * step, step), step)
        wide = a_s[here, :].astype(jnp.float32)
        scale = lax.rsqrt(jnp.mean(wide * wide, -1, keepdims=True) + 1e-6)
        a_s[here, :] = (wide * scale * gain_ref[...].astype(jnp.float32).reshape(1, -1)).astype(jnp.bfloat16)

    def norm():
        x_copy.wait()
        arrived(("swap", "x"), a_s.at[pl.ds(pl.multiple_of((1 - c) * own, 16), own), :])
        lax.fori_loop(0, tokens // step, norm_rows, None)

    def angles():
        place = (z * tokens + lax.broadcasted_iota(jnp.int32, (own, 1), 0)).astype(jnp.float32)
        for i in range(2):
            angle = (place + i * own) * freq_ref[...]
            cos_s[i * own : (i + 1) * own, :] = jnp.cos(angle)
            sin_s[i * own : (i + 1) * own, :] = jnp.sin(angle)

    pass_on("kv", 1)
    share("k", [1])
    set_off("a")
    norm()
    pass_on("kv", 2)
    share("k", [2])
    pass_on("a", 1)
    set_off("bo")
    pass_across("k", [1])
    angles()
    pass_on("kv", 3)
    share("k", [3])
    share("v", [1])
    pass_on("a", 2)
    pass_on("bo", 1)
    pass_across("k", [2])
    pass_on("kv", 4)
    share("k", [4])
    pass_across("k", [3])
    pass_on("a", 3)
    pass_across("k", [4])
    share("v", [2, 3, 4])
    pass_on("bo", 2)

    block = 256

    def project_k(b, _):
        at = pl.ds(pl.multiple_of(b * block, block), block)
        r = _dot(a_s[at, :], wk_s[...], 1, 0).astype(jnp.bfloat16)
        for h in range(kvh):
            k_s[z, h, at, :] = _turn(r[:, h * HEAD : (h + 1) * HEAD], cos_s[at, :], sin_s[at, :])

    def project_v(b, _):
        at = pl.ds(pl.multiple_of(b * block, block), block)
        r = _dot(a_s[at, :], wv_s[...], 1, 0).astype(jnp.bfloat16)
        for h in range(kvh):
            v_s[z, h, :, at] = r[:, h * HEAD : (h + 1) * HEAD].T

    nb = tokens // BK

    def kv_sems(dr, d, h, b, part):
        hb = h * nb + b
        first, later = (dr * kvh * nb + hb) * 2 + part, 4 * kvh * nb + (dr * (far - 1) + d - 2) * kvh * nb + hb
        n = jnp.where(d == 1, first, later) if not isinstance(d, int) else first if d == 1 else later
        return dict(send_sem=kv_send.at[(dr * far + d - 1) * kvh * nb + hb], recv_sem=kv_recv.at[n])

    def kv_copy(dr, d, h, b, part, j, to):
        here = pl.ds(pl.multiple_of(b * BK, BK), BK)
        ref = v_s.at[j, h, :, here] if part else k_s.at[j, h, here, :]
        return pltpu.make_async_remote_copy(src_ref=ref, dst_ref=ref, device_id=to, device_id_type=MESH, **kv_sems(dr, d, h, b, part))

    def kv_both(dr, d, h, b):
        ref = k_s.at[z, h, pl.ds(0, 2 * BK), :]
        return pltpu.make_async_remote_copy(src_ref=ref, dst_ref=ref, device_id=partner, device_id_type=MESH, **kv_sems(dr, d, h, b, 0))

    def made(dr, d, b, at):
        j = jnp.where(dr == PLUS, at - d, at + d)
        j = jnp.where(j >= chips, j - chips, j)
        up = (j >= 0) & (j + d < chips) & ((d < far) | (b == 0))
        down = (j < far) & (((d < far) & (j < far - 1)) | (b == nb - 1))
        return jnp.where(dr == PLUS, up, down) & (d <= far), jnp.where(j < 0, 0, j)

    def next_chip(dr):
        return jnp.where(dr == PLUS, z + 1, (z + chips - 1) % chips)

    def begin(part):
        for h in range(kvh):
            for b in range(nb):
                for dr in (PLUS, MINUS):
                    go, _ = made(dr, 1, b, next_chip(dr))

                    @pl.when(go)
                    def _():
                        kv_copy(dr, 1, h, b, part, z, onward[dr]).start()

    def relay(dr, d, h, b, parts):
        here, j = made(dr, d, b, z)
        nxt = next_chip(dr)
        on, _ = made(dr, d + 1, b, nxt)

        @pl.when(here)
        def _():
            if len(parts) == 1:
                kv_copy(dr, 1, h, b, parts[0], j, partner).wait_recv()
            else:
                kv_both(dr, d, h, b).wait_recv()

            if isinstance(d, int) and d == far:
                return

            @pl.when(on)
            def _():
                for part in parts:
                    kv_copy(dr, d + 1, h, b, part, j, (g, 2 * (nxt % chips) + c)).start()

    complete("k")
    lax.fori_loop(0, tokens // block, project_k, None)
    begin(0)
    pass_on("a", 4)
    pass_on("bo", 3)
    pass_across("v")
    share("a")
    complete("v")
    lax.fori_loop(0, tokens // block, project_v, None)
    begin(1)

    wq_s = [wqa_s, wqb_s]

    def project_q(h):
        def rows_of(b, _):
            at = pl.ds(pl.multiple_of(b * block, block), block)
            r = _dot(a_s[at, :], wq_s[h][...], 1, 0).astype(jnp.bfloat16)
            for n in range(per):
                to = pl.ds(pl.multiple_of(n * tokens + b * block, block), block)
                q_s[h, to, :] = _turn(r[:, n * HEAD : (n + 1) * HEAD], cos_s[at, :], sin_s[at, :])

        lax.fori_loop(0, tokens // block, rows_of, None)

    pass_across("a")
    pass_on("bo", 4)
    share("b")
    complete("a")
    project_q(0)

    def first_hop(i, _):
        part, h, b, dr = i // (2 * nb * kvh), (i // (2 * nb)) % kvh, (i // 2) % nb, i % 2
        n_parts = 2
        for q in range(n_parts):

            @pl.when(part == q)
            def _():
                relay(dr, 1, h, b, [q])

    lax.fori_loop(0, 2 * kvh * nb * 2, first_hop, None)

    pass_across("b")
    share("o")
    complete("b")
    project_q(1)

    e = HEAD**-0.5 * LOG2E
    strips = list(range(0, per * tokens, BK))
    ones = jnp.ones((8, BK), jnp.bfloat16)

    def attend(j, h, b, chosen):
        here = pl.ds(pl.multiple_of(b * BK, BK), BK)
        keys = k_s[j, h, here, :]
        values = jnp.concatenate([v_s[j, h, :, here], ones], axis=0)
        scores = [_dot(keys, q_s[h, at : at + BK, :], 1, 1) for at, _ in chosen]
        weights, keeps = [], []
        for (at, cut), s in zip(chosen, scores):
            if cut:
                s = jnp.where(lax.broadcasted_iota(jnp.int32, s.shape, 1) >= lax.broadcasted_iota(jnp.int32, s.shape, 0), s, HIDDEN)
            old = top_s[h, :, at : at + BK]
            top = jnp.maximum(old, s.max(axis=0, keepdims=True))
            top_s[h, :, at : at + BK] = top
            weights.append(jnp.exp2((s - top) * e).astype(jnp.bfloat16))
            keeps.append(jnp.exp2((old - top) * e))
        for (at, _), w, keep in zip(chosen, weights, keeps):
            mix_s[h, :, at : at + BK] = mix_s[h, :, at : at + BK] * keep + _dot(values, w, 1, 0)

    def own_keys(h, _):
        top_s[h] = jnp.full(top_s.shape[1:], NEG, jnp.float32)
        mix_s[h] = jnp.zeros(mix_s.shape[1:], jnp.float32)
        for b in range(tokens // BK):
            attend(z, h, b, [(at, at % tokens == b * BK) for at in strips if at % tokens >= b * BK])

    lax.fori_loop(0, kvh, own_keys, None)

    wo_copy = copy(("wo",), wo_own, wo_own, partner)

    def left(ds):
        def one(i, _):
            d, h, b, dr = i // (2 * kvh * nb) + ds[0], i // (2 * nb) % kvh, i // 2 % nb, i % 2
            on, _ = made(dr, d, b, next_chip(dr))

            @pl.when(on)
            def _():
                kv_both(dr, d, h, b).wait_send()

        lax.fori_loop(0, len(ds) * 2 * kvh * nb, one, None)

    per_hop = 2 * kvh * nb
    x_again = pltpu.make_async_copy(x_ref, a_s.at[pl.ds(own, own), :], local.at[len(mats)])
    x_again.start()

    def use(dr, d, h, b):
        here, j = made(dr, d, b, z)

        @pl.when(here & (j < z))
        def _():
            attend(j, h, b, [(at, False) for at in strips])

    def hop(i, _):
        d, h, b, dr = i // per_hop + 1, i // (2 * nb) % kvh, i // 2 % nb, i % 2

        @pl.when(i == 2 * per_hop)
        def _():
            pass_across("o")

        @pl.when(d > 1)
        def _():
            relay(dr, d, h, b, [0, 1])

        use(dr, d, h, b)

    lax.fori_loop(0, (far - 1) * per_hop, hop, None)

    complete("o")
    for m in mats:
        gone(m)
    wo_copy.start()
    for t in sent:
        t.wait_send()
    settled = len(sent)
    left(range(1, 3))

    seen = lambda core, h: wq_s[h].at[pl.ds(pl.multiple_of(core * own, 16), own), :]
    stage = lambda _, h: wq_s[h].at[pl.ds(2 * own, own), :]

    def finish(place_of, core, h):
        for n in range(per):
            at = pl.ds(pl.multiple_of(n * tokens + core * own, own), own)
            out = mix_s[h, :HEAD, at] * (1 / mix_s[h, HEAD : HEAD + 1, at])
            place_of(core, h)[:, n * HEAD : (n + 1) * HEAD] = out.T.astype(jnp.bfloat16)

    wide, some = wo_s.shape[2], own // 2
    def patch(i):
        return pl.ds(pl.multiple_of(i % 2 * some, some), some), pl.ds(pl.multiple_of(i // 2 * wide, 128), wide)

    def out_copy(i):
        at, to = patch(i)
        return pltpu.make_async_copy(a_s.at[at, to], y_ref.at[at, to], out_sem.at[i])

    x_again.wait()

    def project(h, cores, first, last):
        deep = wo_s.shape[1] // 2 // kvh

        def one(i, _):
            at, to = patch(i)
            y = a_s[pl.ds(pl.multiple_of(own + i % 2 * some, some), some), to].astype(jnp.float32) if first else sum_s[at, to]
            for core in cores:
                y += _dot(seen(core, h)[at, :], wo_s[i // 2, pl.ds(pl.multiple_of((core * kvh + h) * deep, deep), deep), :], 1, 0)
            if last:
                a_s[at, to] = y.astype(jnp.bfloat16)
                out_copy(i).start()
            else:
                sum_s[at, to] = y

        lax.fori_loop(0, 4, one, None)

    order = list(range(kvh))[::-1]
    for h in order:
        for dr, b in ((PLUS, 0), (MINUS, nb - 1)):
            relay(dr, far, h, b, [0, 1])
            use(dr, far, h, b)
        if h == order[0]:
            arrived(("wo",), wo_s.at[1 - c])
        finish(stage, 1 - c, h)
        finish(seen, c, h)
        start(("seen", h), stage(c, h), seen(c, h), partner)
        if h == order[-1]:
            project(h, [c], False, False)
            arrived(("seen", h), seen(1 - c, h))
            project(h, [1 - c], False, True)
        else:
            arrived(("seen", h), seen(1 - c, h))
            project(h, [c, 1 - c], h == order[0], False)
    lax.fori_loop(0, 4, lambda i, _: out_copy(i).wait(), None)

    wo_copy.wait_send()
    for t in sent[settled:]:
        t.wait_send()
    left(range(3, far + 1))


def solution(mesh):
    chips = mesh.shape["sp"] // 2
    side = math.isqrt(mesh.shape["dp"])

    def step(x, gain, wq, wk, wv, wo):
        own, width = x.shape
        tokens = 2 * own
        half = HEAD // 2
        freq = jnp.asarray(THETA ** (-np.arange(half, dtype=np.float32) / half), jnp.float32).reshape(1, half)
        kvh = wk.shape[1] // HEAD // 2
        per = wq.shape[1] // wk.shape[1]
        far = chips // 2
        vm, hbm = pl.BlockSpec(memory_space=pltpu.VMEM), pl.BlockSpec(memory_space=pl.ANY)
        deep = wo.shape[0] * 2 * chips
        came = 5 * (6 * far + 1) + 5 + 1 + 3
        hops = 2 * (tokens // BK) * kvh
        return pl.pallas_call(
            functools.partial(_kernel, chips, side),
            out_shape=jax.ShapeDtypeStruct((own, width), jnp.bfloat16),
            in_specs=[hbm] + [vm] * 2 + [hbm] * 4,
            out_specs=hbm,
            scratch_shapes=[
                pltpu.VMEM((tokens, width), jnp.bfloat16),
                pltpu.VMEM((width, wk.shape[1] // 2), jnp.bfloat16),
                pltpu.VMEM((width, wv.shape[1] // 2), jnp.bfloat16),
                pltpu.VMEM((width, wq.shape[1] // 4), jnp.bfloat16),
                pltpu.VMEM((width, wq.shape[1] // 4), jnp.bfloat16),
                pltpu.VMEM((2, deep, width // 2), jnp.bfloat16),
                pltpu.VMEM((chips, kvh, tokens, HEAD), jnp.bfloat16),
                pltpu.VMEM((chips, kvh, HEAD, tokens), jnp.bfloat16),
                pltpu.VMEM((kvh, per * tokens, HEAD), jnp.bfloat16),
                pltpu.VMEM((kvh, 1, per * tokens), jnp.float32),
                pltpu.VMEM((kvh, HEAD + 8, per * tokens), jnp.float32),
                pltpu.VMEM((tokens, half), jnp.float32),
                pltpu.VMEM((tokens, half), jnp.float32),
                pltpu.VMEM((own, width), jnp.float32),
                pltpu.SemaphoreType.DMA((5 + 5 + 1 + 3,)),
                pltpu.SemaphoreType.DMA((came,)),
                pltpu.SemaphoreType.DMA((far * hops,)),
                pltpu.SemaphoreType.DMA(((far + 1) * hops,)),
                pltpu.SemaphoreType.DMA((6,)),
                pltpu.SemaphoreType.DMA((4,)),
            ],
            compiler_params=pltpu.CompilerParams(collective_id=0, has_side_effects=True, vmem_limit_bytes=VMEM),
            name="layer",
        )(x, gain, freq, wq, wk, wv, wo)

    tokens, whole = P(("dp", "sp"), None), P("sp", None)
    return jax.shard_map(
        step,
        mesh=mesh,
        in_specs=(tokens, P(None), whole, whole, whole, whole),
        out_specs=tokens,
        check_vma=False,
    )
```

```python
import functools
import math

import jax
import jax.numpy as jnp
import numpy as np
from jax import lax
from jax.experimental import pallas as pl
from jax.experimental.pallas import tpu as pltpu
from jax.sharding import PartitionSpec as P

HEAD = 256
THETA = 10000
NEG = -1e30
HIDDEN = 2 * NEG
LOG2E = 1.4426950408889634
VMEM = 67_000_000
MESH = pl.DeviceIdType.MESH
BK = 512
PLUS, MINUS = 0, 1


def _dot(a, b, ca, cb):
    return lax.dot_general(a, b, (((ca,), (cb,)), ((), ())), preferred_element_type=jnp.float32)


def _turn(t, cos, sin):
    half = t.shape[-1] // 2
    a, b = t[:, :half].astype(jnp.float32), t[:, half:].astype(jnp.float32)
    return jnp.concatenate([a * cos - b * sin, b * cos + a * sin], -1).astype(jnp.bfloat16)


class Ids:
    def __init__(self):
        self.of = {}

    def __call__(self, *key):
        return self.of.setdefault(key, len(self.of))


def _kernel(chips, side, x_ref, gain_ref, freq_ref, wq_ref, wk_ref, wv_ref, wo_ref, y_ref,
            a_s, wk_s, wv_s, wqa_s, wqb_s, wo_s, k_s, v_s, q_s, top_s, mix_s, cos_s, sin_s, sum_s, send, recv, kv_send, kv_recv, local, out_sem):
    own, width = x_ref.shape
    tokens = 2 * own
    kvh = k_s.shape[1]
    per = q_s.shape[1] // tokens
    far = chips // 2
    g, sp = lax.axis_index("dp"), lax.axis_index("sp")
    z, c = sp // 2, sp % 2
    gx, gy = g // side, g % side
    xb, yb = gx % 2, gy % 2
    gx_n = g + (1 - 2 * xb) * side
    gy_n = g + (1 - 2 * yb)
    partner = (g, 2 * z + 1 - c)
    chip_at = lambda dr, d: (z - d + chips) % chips if dr == PLUS else (z + d) % chips
    onward = [(g, 2 * ((z + 1) % chips) + c), (g, 2 * ((z + chips - 1) % chips) + c)]
    beside = {"x": (gx_n, sp), "y": (gy_n, sp)}
    sent_by, came_by = Ids(), Ids()
    sent = []

    def copy(key, src, dst, to):
        name = key[0]
        of_matrix = len(name) < 3 and name[0] in "kvabo"
        s = sent_by(name[0]) if of_matrix else sent_by(*key)
        r = came_by(name) if name[1:] == "d" else came_by(*key)
        return pltpu.make_async_remote_copy(src_ref=src, dst_ref=dst, send_sem=send.at[s], recv_sem=recv.at[r], device_id=to, device_id_type=MESH)

    def start(key, src, dst, to):
        t = copy(key, src, dst, to)
        t.start()
        if len(key[0]) > 2:
            sent.append(t)

    def arrived(key, dst):
        copy(key, dst, dst, partner).wait_recv()

    def rows(w, chip, part, parts, half=None):
        deep = w.shape[0] // chips // parts
        cols = slice(None) if half is None else pl.ds(half * (w.shape[1] // 2), w.shape[1] // 2)
        return w.at[pl.ds(pl.multiple_of(chip * (w.shape[0] // chips) + part * deep, 16), deep), cols]

    wo_own = wo_s.at[c]

    mats = {"k": wk_s, "v": wv_s, "a": wqa_s, "b": wqb_s, "o": wo_own}
    given = {"k": wk_ref, "v": wv_ref, "a": wq_ref, "b": wq_ref, "o": wo_ref}

    def piece(m, core):
        n = mats[m].shape[1]
        first = core * (given[m].shape[1] // 2) + (n if m == "b" else 0)
        return given[m].at[:, pl.ds(pl.multiple_of(first, 128), n)]

    local_copies = {m: pltpu.make_async_copy(piece(m, c), rows(w, z, c, 2), local.at[n]) for n, (m, w) in enumerate(mats.items())}
    mine = pl.ds(pl.multiple_of(c * own, 16), own)
    x_copy = pltpu.make_async_copy(x_ref, a_s.at[mine, :], local.at[len(mats)])
    for t in [*local_copies.values(), x_copy]:
        t.start()

    barrier = pltpu.get_barrier_semaphore()
    around = [*onward, *beside.values(), partner]
    for who in around:
        pl.semaphore_signal(barrier, inc=1, device_id=who, device_id_type=MESH)
    pl.semaphore_wait(barrier, len(around))

    for m in mats:
        target = wo_s.at[1 - c] if m == "o" else mats[m]
        start(("swap", m), piece(m, 1 - c), rows(target, z, c, 2), partner)
        if m == "v":
            start(("swap", "x"), x_ref, a_s.at[mine, :], partner)

    quarter = 2 * xb + yb
    quarters = {"x": 2 * (1 - xb) + yb, "y": 2 * xb + 1 - yb, "d": 2 * (1 - xb) + 1 - yb}
    half_of = lambda dr, d: None if d < far else dr
    hops = [(dr, d) for d in range(1, far + 1) for dr in (PLUS, MINUS)]

    def set_off(names):
        for m in names:
            local_copies[m].wait()
            arrived(("swap", m), rows(mats[m], z, 1 - c, 2))
        for m in names:
            for dr in (PLUS, MINUS):
                r = rows(mats[m], z, quarter, 4)
                start((m, dr, 1), r, r, onward[dr])

    def pass_on(names, d):
        for dr in (PLUS, MINUS):
            for m in names:
                r = rows(mats[m], chip_at(dr, d), quarter, 4, half_of(dr, d))
                arrived((m, dr, d), r)
                if d < far:
                    f = rows(mats[m], chip_at(dr, d), quarter, 4, half_of(dr, d + 1))
                    start((m, dr, d + 1), f, f, onward[dr])

    everywhere = range(1, far + 1)

    def share(m, ds=everywhere):
        for d in ds:
            for dr in (PLUS, MINUS):
                r = rows(mats[m], chip_at(dr, d), quarter, 4, half_of(dr, d))
                for way in ("x", "y"):
                    start((m + way, dr, d), r, r, beside[way])

    def across(m, d, dr):
        for side_, way, to in ((PLUS, "x", "y"), (MINUS, "y", "x")):
            if d < far or dr == side_:
                yield side_, way, to

    def pass_across(m, ds=everywhere):
        for d in ds:
            for dr in (PLUS, MINUS):
                for way in ("x", "y"):
                    arrived((m + way, dr, d), rows(mats[m], chip_at(dr, d), quarters[way], 4, half_of(dr, d)))
                for side_, way, to in across(m, d, dr):
                    r = rows(mats[m], chip_at(dr, d), quarters[way], 4, side_)
                    start((m + "d", dr, d, side_), r, r, beside[to])

    def top_of(m, n):
        return mats[m].at[pl.ds(0, mats[m].shape[0] // (4 * chips) * n), :]

    pieces = 2 * far - 1

    def complete(m):
        arrived((m + "d",), top_of(m, pieces))

    def gone(m):
        t = top_of(m, 4 * pieces)
        copy((m, PLUS, 1), t, t, partner).wait_send()

    set_off("kv")

    step = 64

    def norm_rows(i, _):
        here = pl.ds(pl.multiple_of(i * step, step), step)
        wide = a_s[here, :].astype(jnp.float32)
        scale = lax.rsqrt(jnp.mean(wide * wide, -1, keepdims=True) + 1e-6)
        a_s[here, :] = (wide * scale * gain_ref[...].astype(jnp.float32).reshape(1, -1)).astype(jnp.bfloat16)

    def norm():
        x_copy.wait()
        arrived(("swap", "x"), a_s.at[pl.ds(pl.multiple_of((1 - c) * own, 16), own), :])
        lax.fori_loop(0, tokens // step, norm_rows, None)

    def angles():
        place = (z * tokens + lax.broadcasted_iota(jnp.int32, (own, 1), 0)).astype(jnp.float32)
        for i in range(2):
            angle = (place + i * own) * freq_ref[...]
            cos_s[i * own : (i + 1) * own, :] = jnp.cos(angle)
            sin_s[i * own : (i + 1) * own, :] = jnp.sin(angle)

    pass_on("kv", 1)
    share("k", [1])
    set_off("a")
    norm()
    pass_on("kv", 2)
    share("k", [2])
    pass_on("a", 1)
    set_off("bo")
    pass_across("k", [1])
    angles()
    pass_on("kv", 3)
    share("k", [3])
    share("v", [1])
    pass_on("a", 2)
    pass_on("bo", 1)
    pass_across("k", [2])
    pass_on("kv", 4)
    share("k", [4])
    pass_across("k", [3])
    pass_on("a", 3)
    pass_across("k", [4])
    share("v", [2, 3, 4])
    pass_on("bo", 2)

    block = 256

    def project_k(b, _):
        at = pl.ds(pl.multiple_of(b * block, block), block)
        r = _dot(a_s[at, :], wk_s[...], 1, 0).astype(jnp.bfloat16)
        for h in range(kvh):
            k_s[z, h, at, :] = _turn(r[:, h * HEAD : (h + 1) * HEAD], cos_s[at, :], sin_s[at, :])

    def project_v(b, _):
        at = pl.ds(pl.multiple_of(b * block, block), block)
        r = _dot(a_s[at, :], wv_s[...], 1, 0).astype(jnp.bfloat16)
        for h in range(kvh):
            v_s[z, h, :, at] = r[:, h * HEAD : (h + 1) * HEAD].T

    nb = tokens // BK

    def kv_sems(dr, d, h, b, part):
        hb = h * nb + b
        first, later = (dr * kvh * nb + hb) * 2 + part, 4 * kvh * nb + (dr * (far - 1) + d - 2) * kvh * nb + hb
        n = jnp.where(d == 1, first, later) if not isinstance(d, int) else first if d == 1 else later
        return dict(send_sem=kv_send.at[(dr * far + d - 1) * kvh * nb + hb], recv_sem=kv_recv.at[n])

    def kv_copy(dr, d, h, b, part, j, to):
        here = pl.ds(pl.multiple_of(b * BK, BK), BK)
        ref = v_s.at[j, h, :, here] if part else k_s.at[j, h, here, :]
        return pltpu.make_async_remote_copy(src_ref=ref, dst_ref=ref, device_id=to, device_id_type=MESH, **kv_sems(dr, d, h, b, part))

    def kv_both(dr, d, h, b):
        ref = k_s.at[z, h, pl.ds(0, 2 * BK), :]
        return pltpu.make_async_remote_copy(src_ref=ref, dst_ref=ref, device_id=partner, device_id_type=MESH, **kv_sems(dr, d, h, b, 0))

    def made(dr, d, b, at):
        j = jnp.where(dr == PLUS, at - d, at + d)
        j = jnp.where(j >= chips, j - chips, j)
        up = (j >= 0) & (j + d < chips) & ((d < far) | (b == 0))
        down = (j < far) & (((d < far) & (j < far - 1)) | (b == nb - 1))
        return jnp.where(dr == PLUS, up, down) & (d <= far), jnp.where(j < 0, 0, j)

    def next_chip(dr):
        return jnp.where(dr == PLUS, z + 1, (z + chips - 1) % chips)

    def begin(part):
        for h in range(kvh):
            for b in range(nb):
                for dr in (PLUS, MINUS):
                    go, _ = made(dr, 1, b, next_chip(dr))

                    @pl.when(go)
                    def _():
                        kv_copy(dr, 1, h, b, part, z, onward[dr]).start()

    def relay(dr, d, h, b, parts):
        here, j = made(dr, d, b, z)
        nxt = next_chip(dr)
        on, _ = made(dr, d + 1, b, nxt)

        @pl.when(here)
        def _():
            if len(parts) == 1:
                kv_copy(dr, 1, h, b, parts[0], j, partner).wait_recv()
            else:
                kv_both(dr, d, h, b).wait_recv()

            if isinstance(d, int) and d == far:
                return

            @pl.when(on)
            def _():
                for part in parts:
                    kv_copy(dr, d + 1, h, b, part, j, (g, 2 * (nxt % chips) + c)).start()

    complete("k")
    lax.fori_loop(0, tokens // block, project_k, None)
    begin(0)
    pass_on("a", 4)
    pass_on("bo", 3)
    pass_across("v")
    share("a")
    complete("v")
    lax.fori_loop(0, tokens // block, project_v, None)
    begin(1)

    wq_s = [wqa_s, wqb_s]

    def project_q(h):
        def rows_of(b, _):
            at = pl.ds(pl.multiple_of(b * block, block), block)
            r = _dot(a_s[at, :], wq_s[h][...], 1, 0).astype(jnp.bfloat16)
            for n in range(per):
                to = pl.ds(pl.multiple_of(n * tokens + b * block, block), block)
                q_s[h, to, :] = _turn(r[:, n * HEAD : (n + 1) * HEAD], cos_s[at, :], sin_s[at, :])

        lax.fori_loop(0, tokens // block, rows_of, None)

    def first_hop(part):
        def one(i, _):
            relay(i % 2, 1, i // (2 * nb), (i // 2) % nb, [part])

        lax.fori_loop(0, 2 * kvh * nb, one, None)

    pass_across("a", [1, 2])
    first_hop(0)
    pass_across("a", [3, 4])
    pass_on("bo", 4)
    share("b")
    complete("a")
    project_q(0)

    first_hop(1)

    pass_across("b")
    share("o")
    complete("b")
    project_q(1)

    e = HEAD**-0.5 * LOG2E
    strips = list(range(0, per * tokens, BK))
    ones = jnp.ones((8, BK), jnp.bfloat16)

    def attend(j, h, b, chosen):
        here = pl.ds(pl.multiple_of(b * BK, BK), BK)
        keys = k_s[j, h, here, :]
        values = jnp.concatenate([v_s[j, h, :, here], ones], axis=0)
        scores = [_dot(keys, q_s[h, at : at + BK, :], 1, 1) for at, _ in chosen]
        weights, keeps = [], []
        for (at, cut), s in zip(chosen, scores):
            if cut:
                s = jnp.where(lax.broadcasted_iota(jnp.int32, s.shape, 1) >= lax.broadcasted_iota(jnp.int32, s.shape, 0), s, HIDDEN)
            old = top_s[h, :, at : at + BK]
            top = jnp.maximum(old, s.max(axis=0, keepdims=True))
            top_s[h, :, at : at + BK] = top
            weights.append(jnp.exp2((s - top) * e).astype(jnp.bfloat16))
            keeps.append(jnp.exp2((old - top) * e))
        for (at, _), w, keep in zip(chosen, weights, keeps):
            mix_s[h, :, at : at + BK] = mix_s[h, :, at : at + BK] * keep + _dot(values, w, 1, 0)

    def own_keys(h, _):
        top_s[h] = jnp.full(top_s.shape[1:], NEG, jnp.float32)
        mix_s[h] = jnp.zeros(mix_s.shape[1:], jnp.float32)
        for b in range(tokens // BK):
            attend(z, h, b, [(at, at % tokens == b * BK) for at in strips if at % tokens >= b * BK])

    lax.fori_loop(0, kvh, own_keys, None)

    wo_copy = copy(("wo",), wo_own, wo_own, partner)

    def left(ds):
        def one(i, _):
            d, h, b, dr = i // (2 * kvh * nb) + ds[0], i // (2 * nb) % kvh, i // 2 % nb, i % 2
            on, _ = made(dr, d, b, next_chip(dr))

            @pl.when(on)
            def _():
                kv_both(dr, d, h, b).wait_send()

        lax.fori_loop(0, len(ds) * 2 * kvh * nb, one, None)

    per_hop = 2 * kvh * nb
    x_again = pltpu.make_async_copy(x_ref, a_s.at[pl.ds(own, own), :], local.at[len(mats)])
    x_again.start()

    def use(dr, d, h, b):
        here, j = made(dr, d, b, z)

        @pl.when(here & (j < z))
        def _():
            attend(j, h, b, [(at, False) for at in strips])

    def hop(i, _):
        d, h, b, dr = i // per_hop + 1, i // (2 * nb) % kvh, i // 2 % nb, i % 2

        @pl.when(i == 2 * per_hop)
        def _():
            pass_across("o")

        @pl.when(d > 1)
        def _():
            relay(dr, d, h, b, [0, 1])

        use(dr, d, h, b)

    lax.fori_loop(0, (far - 1) * per_hop, hop, None)

    complete("o")
    for m in mats:
        gone(m)
    wo_copy.start()
    for t in sent:
        t.wait_send()
    settled = len(sent)
    left(range(1, 3))

    seen = lambda core, h: wq_s[h].at[pl.ds(pl.multiple_of(core * own, 16), own), :]
    stage = lambda _, h: wq_s[h].at[pl.ds(2 * own, own), :]

    def finish(place_of, core, h):
        for n in range(per):
            at = pl.ds(pl.multiple_of(n * tokens + core * own, own), own)
            out = mix_s[h, :HEAD, at] * (1 / mix_s[h, HEAD : HEAD + 1, at])
            place_of(core, h)[:, n * HEAD : (n + 1) * HEAD] = out.T.astype(jnp.bfloat16)

    wide, some = wo_s.shape[2], own // 2
    def patch(i):
        return pl.ds(pl.multiple_of(i % 2 * some, some), some), pl.ds(pl.multiple_of(i // 2 * wide, 128), wide)

    def out_copy(i):
        at, to = patch(i)
        return pltpu.make_async_copy(a_s.at[at, to], y_ref.at[at, to], out_sem.at[i])

    x_again.wait()

    def project(h, cores, first, last):
        deep = wo_s.shape[1] // 2 // kvh

        def one(i, _):
            at, to = patch(i)
            y = a_s[pl.ds(pl.multiple_of(own + i % 2 * some, some), some), to].astype(jnp.float32) if first else sum_s[at, to]
            for core in cores:
                y += _dot(seen(core, h)[at, :], wo_s[i // 2, pl.ds(pl.multiple_of((core * kvh + h) * deep, deep), deep), :], 1, 0)
            if last:
                a_s[at, to] = y.astype(jnp.bfloat16)
                out_copy(i).start()
            else:
                sum_s[at, to] = y

        lax.fori_loop(0, 4, one, None)

    order = list(range(kvh))
    for h in order:
        for dr, b in ((PLUS, 0), (MINUS, nb - 1)):
            relay(dr, far, h, b, [0, 1])
            use(dr, far, h, b)
        if h == order[0]:
            arrived(("wo",), wo_s.at[1 - c])
        finish(stage, 1 - c, h)
        finish(seen, c, h)
        start(("seen", h), stage(c, h), seen(c, h), partner)
        if h == order[-1]:
            project(h, [c], False, False)
            arrived(("seen", h), seen(1 - c, h))
            project(h, [1 - c], False, True)
        else:
            arrived(("seen", h), seen(1 - c, h))
            project(h, [c, 1 - c], h == order[0], False)
    lax.fori_loop(0, 4, lambda i, _: out_copy(i).wait(), None)

    wo_copy.wait_send()
    for t in sent[settled:]:
        t.wait_send()
    left(range(3, far + 1))


def solution(mesh):
    chips = mesh.shape["sp"] // 2
    side = math.isqrt(mesh.shape["dp"])

    def step(x, gain, wq, wk, wv, wo):
        own, width = x.shape
        tokens = 2 * own
        half = HEAD // 2
        freq = jnp.asarray(THETA ** (-np.arange(half, dtype=np.float32) / half), jnp.float32).reshape(1, half)
        kvh = wk.shape[1] // HEAD // 2
        per = wq.shape[1] // wk.shape[1]
        far = chips // 2
        vm, hbm = pl.BlockSpec(memory_space=pltpu.VMEM), pl.BlockSpec(memory_space=pl.ANY)
        deep = wo.shape[0] * 2 * chips
        came = 5 * (6 * far + 1) + 5 + 1 + 3
        hops = 2 * (tokens // BK) * kvh
        return pl.pallas_call(
            functools.partial(_kernel, chips, side),
            out_shape=jax.ShapeDtypeStruct((own, width), jnp.bfloat16),
            in_specs=[hbm] + [vm] * 2 + [hbm] * 4,
            out_specs=hbm,
            scratch_shapes=[
                pltpu.VMEM((tokens, width), jnp.bfloat16),
                pltpu.VMEM((width, wk.shape[1] // 2), jnp.bfloat16),
                pltpu.VMEM((width, wv.shape[1] // 2), jnp.bfloat16),
                pltpu.VMEM((width, wq.shape[1] // 4), jnp.bfloat16),
                pltpu.VMEM((width, wq.shape[1] // 4), jnp.bfloat16),
                pltpu.VMEM((2, deep, width // 2), jnp.bfloat16),
                pltpu.VMEM((chips, kvh, tokens, HEAD), jnp.bfloat16),
                pltpu.VMEM((chips, kvh, HEAD, tokens), jnp.bfloat16),
                pltpu.VMEM((kvh, per * tokens, HEAD), jnp.bfloat16),
                pltpu.VMEM((kvh, 1, per * tokens), jnp.float32),
                pltpu.VMEM((kvh, HEAD + 8, per * tokens), jnp.float32),
                pltpu.VMEM((tokens, half), jnp.float32),
                pltpu.VMEM((tokens, half), jnp.float32),
                pltpu.VMEM((own, width), jnp.float32),
                pltpu.SemaphoreType.DMA((5 + 5 + 1 + 3,)),
                pltpu.SemaphoreType.DMA((came,)),
                pltpu.SemaphoreType.DMA((far * hops,)),
                pltpu.SemaphoreType.DMA(((far + 1) * hops,)),
                pltpu.SemaphoreType.DMA((6,)),
                pltpu.SemaphoreType.DMA((4,)),
            ],
            compiler_params=pltpu.CompilerParams(collective_id=0, has_side_effects=True, vmem_limit_bytes=VMEM),
            name="layer",
        )(x, gain, freq, wq, wk, wv, wo)

    tokens, whole = P(("dp", "sp"), None), P("sp", None)
    return jax.shard_map(
        step,
        mesh=mesh,
        in_specs=(tokens, P(None), whole, whole, whole, whole),
        out_specs=tokens,
        check_vma=False,
    )
```

```python
import functools
import math

import jax
import jax.numpy as jnp
import numpy as np
from jax import lax
from jax.experimental import pallas as pl
from jax.experimental.pallas import tpu as pltpu
from jax.sharding import PartitionSpec as P

HEAD = 256
THETA = 10000
NEG = -1e30
HIDDEN = 2 * NEG
LOG2E = 1.4426950408889634
VMEM = 67_000_000
MESH = pl.DeviceIdType.MESH
BK = 512
PLUS, MINUS = 0, 1


def _dot(a, b, ca, cb):
    return lax.dot_general(a, b, (((ca,), (cb,)), ((), ())), preferred_element_type=jnp.float32)


def _turn(t, cos, sin):
    half = t.shape[-1] // 2
    a, b = t[:, :half].astype(jnp.float32), t[:, half:].astype(jnp.float32)
    return jnp.concatenate([a * cos - b * sin, b * cos + a * sin], -1).astype(jnp.bfloat16)


class Ids:
    def __init__(self):
        self.of = {}

    def __call__(self, *key):
        return self.of.setdefault(key, len(self.of))


def _kernel(chips, side, x_ref, gain_ref, freq_ref, wq_ref, wk_ref, wv_ref, wo_ref, y_ref,
            a_s, wk_s, wv_s, wqa_s, wqb_s, wo_s, k_s, v_s, q_s, top_s, mix_s, cos_s, sin_s, sum_s, send, recv, kv_send, kv_recv, local, out_sem):
    own, width = x_ref.shape
    tokens = 2 * own
    kvh = k_s.shape[1]
    per = q_s.shape[1] // tokens
    far = chips // 2
    g, sp = lax.axis_index("dp"), lax.axis_index("sp")
    z, c = sp // 2, sp % 2
    gx, gy = g // side, g % side
    xb, yb = gx % 2, gy % 2
    gx_n = g + (1 - 2 * xb) * side
    gy_n = g + (1 - 2 * yb)
    partner = (g, 2 * z + 1 - c)
    chip_at = lambda dr, d: (z - d + chips) % chips if dr == PLUS else (z + d) % chips
    onward = [(g, 2 * ((z + 1) % chips) + c), (g, 2 * ((z + chips - 1) % chips) + c)]
    beside = {"x": (gx_n, sp), "y": (gy_n, sp)}
    sent_by, came_by = Ids(), Ids()
    sent = []

    def copy(key, src, dst, to):
        name = key[0]
        of_matrix = len(name) < 3 and name[0] in "kvabo"
        s = sent_by(name[0]) if of_matrix else sent_by(*key)
        r = came_by(name) if name[1:] == "d" else came_by(name[0] + "xy", *key[1:]) if name[1:] in ("x", "y") else came_by(*key)
        return pltpu.make_async_remote_copy(src_ref=src, dst_ref=dst, send_sem=send.at[s], recv_sem=recv.at[r], device_id=to, device_id_type=MESH)

    def start(key, src, dst, to):
        t = copy(key, src, dst, to)
        t.start()
        if len(key[0]) > 2:
            sent.append(t)

    def arrived(key, dst):
        copy(key, dst, dst, partner).wait_recv()

    def rows(w, chip, part, parts, half=None):
        deep = w.shape[0] // chips // parts
        cols = slice(None) if half is None else pl.ds(half * (w.shape[1] // 2), w.shape[1] // 2)
        return w.at[pl.ds(pl.multiple_of(chip * (w.shape[0] // chips) + part * deep, 16), deep), cols]

    wo_own = wo_s.at[c]

    mats = {"k": wk_s, "v": wv_s, "a": wqa_s, "b": wqb_s, "o": wo_own}
    given = {"k": wk_ref, "v": wv_ref, "a": wq_ref, "b": wq_ref, "o": wo_ref}

    def piece(m, core):
        n = mats[m].shape[1]
        first = core * (given[m].shape[1] // 2) + (n if m == "b" else 0)
        return given[m].at[:, pl.ds(pl.multiple_of(first, 128), n)]

    local_copies = {m: pltpu.make_async_copy(piece(m, c), rows(w, z, c, 2), local.at[n]) for n, (m, w) in enumerate(mats.items())}
    mine = pl.ds(pl.multiple_of(c * own, 16), own)
    x_copy = pltpu.make_async_copy(x_ref, a_s.at[mine, :], local.at[len(mats)])
    for t in [*local_copies.values(), x_copy]:
        t.start()

    barrier = pltpu.get_barrier_semaphore()
    around = [*onward, *beside.values(), partner]
    for who in around:
        pl.semaphore_signal(barrier, inc=1, device_id=who, device_id_type=MESH)
    pl.semaphore_wait(barrier, len(around))

    for m in mats:
        target = wo_s.at[1 - c] if m == "o" else mats[m]
        start(("swap", m), piece(m, 1 - c), rows(target, z, c, 2), partner)
        if m == "v":
            start(("swap", "x"), x_ref, a_s.at[mine, :], partner)

    quarter = 2 * xb + yb
    quarters = {"x": 2 * (1 - xb) + yb, "y": 2 * xb + 1 - yb, "d": 2 * (1 - xb) + 1 - yb}
    half_of = lambda dr, d: None if d < far else dr
    hops = [(dr, d) for d in range(1, far + 1) for dr in (PLUS, MINUS)]

    def set_off(names):
        for m in names:
            local_copies[m].wait()
            arrived(("swap", m), rows(mats[m], z, 1 - c, 2))
        for m in names:
            for dr in (PLUS, MINUS):
                r = rows(mats[m], z, quarter, 4)
                start((m, dr, 1), r, r, onward[dr])

    def pass_on(names, d):
        for dr in (PLUS, MINUS):
            for m in names:
                r = rows(mats[m], chip_at(dr, d), quarter, 4, half_of(dr, d))
                arrived((m, dr, d), r)
                if d < far:
                    f = rows(mats[m], chip_at(dr, d), quarter, 4, half_of(dr, d + 1))
                    start((m, dr, d + 1), f, f, onward[dr])

    everywhere = range(1, far + 1)

    def share(m, ds=everywhere):
        for d in ds:
            for dr in (PLUS, MINUS):
                r = rows(mats[m], chip_at(dr, d), quarter, 4, half_of(dr, d))
                for way in ("x", "y"):
                    start((m + way, dr, d), r, r, beside[way])

    def across(m, d, dr):
        for side_, way, to in ((PLUS, "x", "y"), (MINUS, "y", "x")):
            if d < far or dr == side_:
                yield side_, way, to

    def top_of(m, n):
        return mats[m].at[pl.ds(0, mats[m].shape[0] // (4 * chips) * n), :]

    def pass_across(m, ds=everywhere):
        for d in ds:
            for dr in (PLUS, MINUS):
                arrived((m + "x", dr, d), top_of(m, 2 if d < far else 1))
                for side_, way, to in across(m, d, dr):
                    r = rows(mats[m], chip_at(dr, d), quarters[way], 4, side_)
                    start((m + "d", dr, d, side_), r, r, beside[to])

    pieces = 2 * far - 1

    def complete(m):
        arrived((m + "d",), top_of(m, pieces))

    def gone(m):
        t = top_of(m, 4 * pieces)
        copy((m, PLUS, 1), t, t, partner).wait_send()

    set_off("kv")

    step = 64

    def norm_rows(i, _):
        here = pl.ds(pl.multiple_of(i * step, step), step)
        wide = a_s[here, :].astype(jnp.float32)
        scale = lax.rsqrt(jnp.mean(wide * wide, -1, keepdims=True) + 1e-6)
        a_s[here, :] = (wide * scale * gain_ref[...].astype(jnp.float32).reshape(1, -1)).astype(jnp.bfloat16)

    def norm():
        x_copy.wait()
        arrived(("swap", "x"), a_s.at[pl.ds(pl.multiple_of((1 - c) * own, 16), own), :])
        lax.fori_loop(0, tokens // step, norm_rows, None)

    def angles():
        place = (z * tokens + lax.broadcasted_iota(jnp.int32, (own, 1), 0)).astype(jnp.float32)
        for i in range(2):
            angle = (place + i * own) * freq_ref[...]
            cos_s[i * own : (i + 1) * own, :] = jnp.cos(angle)
            sin_s[i * own : (i + 1) * own, :] = jnp.sin(angle)

    pass_on("kv", 1)
    share("k", [1])
    set_off("a")
    norm()
    pass_on("kv", 2)
    share("k", [2])
    pass_on("a", 1)
    set_off("b")
    pass_across("k", [1])
    angles()
    pass_on("kv", 3)
    share("k", [3])
    pass_on("a", 2)
    set_off("o")
    pass_across("k", [2])
    pass_on("kv", 4)
    share("k", [4])
    pass_across("k", [3])
    pass_on("b", 1)
    pass_on("a", 3)
    pass_across("k", [4])
    share("v")
    pass_on("b", 2)
    pass_on("o", 1)

    block = 256

    def project_k(b, _):
        at = pl.ds(pl.multiple_of(b * block, block), block)
        r = _dot(a_s[at, :], wk_s[...], 1, 0).astype(jnp.bfloat16)
        for h in range(kvh):
            k_s[z, h, at, :] = _turn(r[:, h * HEAD : (h + 1) * HEAD], cos_s[at, :], sin_s[at, :])

    def project_v(b, _):
        at = pl.ds(pl.multiple_of(b * block, block), block)
        r = _dot(a_s[at, :], wv_s[...], 1, 0).astype(jnp.bfloat16)
        for h in range(kvh):
            v_s[z, h, :, at] = r[:, h * HEAD : (h + 1) * HEAD].T

    nb = tokens // BK

    def kv_sems(dr, d, h, b, part):
        hb = h * nb + b
        first, later = (dr * kvh * nb + hb) * 2 + part, 4 * kvh * nb + (dr * (far - 1) + d - 2) * kvh * nb + hb
        n = jnp.where(d == 1, first, later) if not isinstance(d, int) else first if d == 1 else later
        return dict(send_sem=kv_send.at[(dr * far + d - 1) * kvh * nb + hb], recv_sem=kv_recv.at[n])

    def kv_copy(dr, d, h, b, part, j, to):
        here = pl.ds(pl.multiple_of(b * BK, BK), BK)
        ref = v_s.at[j, h, :, here] if part else k_s.at[j, h, here, :]
        return pltpu.make_async_remote_copy(src_ref=ref, dst_ref=ref, device_id=to, device_id_type=MESH, **kv_sems(dr, d, h, b, part))

    def kv_both(dr, d, h, b):
        ref = k_s.at[z, h, pl.ds(0, 2 * BK), :]
        return pltpu.make_async_remote_copy(src_ref=ref, dst_ref=ref, device_id=partner, device_id_type=MESH, **kv_sems(dr, d, h, b, 0))

    def made(dr, d, b, at):
        j = jnp.where(dr == PLUS, at - d, at + d)
        j = jnp.where(j >= chips, j - chips, j)
        up = (j >= 0) & (j + d < chips) & ((d < far) | ((j > 0) & (b == 0)))
        down = (j < far) & ((((d < far) | (j == 0)) & (j < far - 1)) | (b == nb - 1))
        return jnp.where(dr == PLUS, up, down) & (d <= far), jnp.where(j < 0, 0, j)

    def next_chip(dr):
        return jnp.where(dr == PLUS, z + 1, (z + chips - 1) % chips)

    def begin(part):
        for h in range(kvh):
            for b in range(nb):
                for dr in (PLUS, MINUS):
                    go, _ = made(dr, 1, b, next_chip(dr))

                    @pl.when(go)
                    def _():
                        kv_copy(dr, 1, h, b, part, z, onward[dr]).start()

    def relay(dr, d, h, b, parts):
        here, j = made(dr, d, b, z)
        nxt = next_chip(dr)
        on, _ = made(dr, d + 1, b, nxt)

        @pl.when(here)
        def _():
            if len(parts) == 1:
                kv_copy(dr, 1, h, b, parts[0], j, partner).wait_recv()
            else:
                kv_both(dr, d, h, b).wait_recv()

            if isinstance(d, int) and d == far:
                return

            @pl.when(on)
            def _():
                for part in parts:
                    kv_copy(dr, d + 1, h, b, part, j, (g, 2 * (nxt % chips) + c)).start()

    complete("k")
    lax.fori_loop(0, tokens // block, project_k, None)
    begin(0)
    pass_on("a", 4)
    pass_on("b", 3)
    pass_on("o", 2)
    pass_across("v")
    share("a")
    complete("v")
    lax.fori_loop(0, tokens // block, project_v, None)
    begin(1)

    wq_s = [wqa_s, wqb_s]

    def project_q(h):
        def rows_of(b, _):
            at = pl.ds(pl.multiple_of(b * block, block), block)
            r = _dot(a_s[at, :], wq_s[h][...], 1, 0).astype(jnp.bfloat16)
            for n in range(per):
                to = pl.ds(pl.multiple_of(n * tokens + b * block, block), block)
                q_s[h, to, :] = _turn(r[:, n * HEAD : (n + 1) * HEAD], cos_s[at, :], sin_s[at, :])

        lax.fori_loop(0, tokens // block, rows_of, None)

    def first_hop(part):
        def one(i, _):
            relay(i % 2, 1, i // (2 * nb), (i // 2) % nb, [part])

        lax.fori_loop(0, 2 * kvh * nb, one, None)

    pass_across("a", [1, 2])
    first_hop(0)
    pass_across("a", [3, 4])
    pass_on("b", 4)
    pass_on("o", 3)
    share("b")
    complete("a")
    project_q(0)

    first_hop(1)

    pass_across("b")
    share("o", [1, 2, 3])
    complete("b")
    project_q(1)

    e = HEAD**-0.5 * LOG2E
    strips = list(range(0, per * tokens, BK))
    ones = jnp.ones((8, BK), jnp.bfloat16)

    def attend(j, h, b, chosen):
        here = pl.ds(pl.multiple_of(b * BK, BK), BK)
        keys = k_s[j, h, here, :]
        values = jnp.concatenate([v_s[j, h, :, here], ones], axis=0)
        scores = [_dot(keys, q_s[h, at : at + BK, :], 1, 1) for at, _ in chosen]
        weights, keeps = [], []
        for (at, cut), s in zip(chosen, scores):
            if cut:
                s = jnp.where(lax.broadcasted_iota(jnp.int32, s.shape, 1) >= lax.broadcasted_iota(jnp.int32, s.shape, 0), s, HIDDEN)
            old = top_s[h, :, at : at + BK]
            top = jnp.maximum(old, s.max(axis=0, keepdims=True))
            top_s[h, :, at : at + BK] = top
            weights.append(jnp.exp2((s - top) * e).astype(jnp.bfloat16))
            keeps.append(jnp.exp2((old - top) * e))
        for (at, _), w, keep in zip(chosen, weights, keeps):
            mix_s[h, :, at : at + BK] = mix_s[h, :, at : at + BK] * keep + _dot(values, w, 1, 0)

    def own_keys(h, _):
        top_s[h] = jnp.full(top_s.shape[1:], NEG, jnp.float32)
        mix_s[h] = jnp.zeros(mix_s.shape[1:], jnp.float32)
        for b in range(tokens // BK):
            attend(z, h, b, [(at, at % tokens == b * BK) for at in strips if at % tokens >= b * BK])

    lax.fori_loop(0, kvh, own_keys, None)

    wo_copy = copy(("wo",), wo_own, wo_own, partner)

    def left(ds):
        def one(i, _):
            d, h, b, dr = i // (2 * kvh * nb) + ds[0], i // (2 * nb) % kvh, i // 2 % nb, i % 2
            on, _ = made(dr, d, b, next_chip(dr))

            @pl.when(on)
            def _():
                kv_both(dr, d, h, b).wait_send()

        lax.fori_loop(0, len(ds) * 2 * kvh * nb, one, None)

    per_hop = 2 * kvh * nb
    x_again = pltpu.make_async_copy(x_ref, a_s.at[pl.ds(own, own), :], local.at[len(mats)])
    x_again.start()

    def use(dr, d, h, b):
        here, j = made(dr, d, b, z)

        @pl.when(here & (j < z))
        def _():
            attend(j, h, b, [(at, False) for at in strips])

    def hop(i, _):
        d, h, b, dr = i // per_hop + 1, i // (2 * nb) % kvh, i // 2 % nb, i % 2

        @pl.when(i == per_hop)
        def _():
            pass_on("o", far)
            share("o", [far])

        @pl.when(i == 2 * per_hop)
        def _():
            pass_across("o")

        @pl.when(d > 1)
        def _():
            relay(dr, d, h, b, [0, 1])

        use(dr, d, h, b)

    lax.fori_loop(0, (far - 1) * per_hop, hop, None)

    complete("o")
    for m in mats:
        gone(m)
    wo_copy.start()
    for t in sent:
        t.wait_send()
    settled = len(sent)
    left(range(1, 3))

    seen = lambda core, h: wq_s[h].at[pl.ds(pl.multiple_of(core * own, 16), own), :]
    stage = lambda _, h: wq_s[h].at[pl.ds(2 * own, own), :]

    def finish(place_of, core, h):
        for n in range(per):
            at = pl.ds(pl.multiple_of(n * tokens + core * own, own), own)
            out = mix_s[h, :HEAD, at] * (1 / mix_s[h, HEAD : HEAD + 1, at])
            place_of(core, h)[:, n * HEAD : (n + 1) * HEAD] = out.T.astype(jnp.bfloat16)

    wide, some = wo_s.shape[2], own // 2
    def patch(i):
        return pl.ds(pl.multiple_of(i % 2 * some, some), some), pl.ds(pl.multiple_of(i // 2 * wide, 128), wide)

    def out_copy(i):
        at, to = patch(i)
        return pltpu.make_async_copy(a_s.at[at, to], y_ref.at[at, to], out_sem.at[i])

    x_again.wait()

    def project(h, cores, first, last):
        deep = wo_s.shape[1] // 2 // kvh

        def one(i, _):
            at, to = patch(i)
            y = a_s[pl.ds(pl.multiple_of(own + i % 2 * some, some), some), to].astype(jnp.float32) if first else sum_s[at, to]
            for core in cores:
                y += _dot(seen(core, h)[at, :], wo_s[i // 2, pl.ds(pl.multiple_of((core * kvh + h) * deep, deep), deep), :], 1, 0)
            if last:
                a_s[at, to] = y.astype(jnp.bfloat16)
                out_copy(i).start()
            else:
                sum_s[at, to] = y

        lax.fori_loop(0, 4, one, None)

    order = list(range(kvh))
    for h in order:
        for dr, b in ((MINUS, 0), (PLUS, 0), (MINUS, nb - 1)):
            relay(dr, far, h, b, [0, 1])
            use(dr, far, h, b)
        if h == order[0]:
            arrived(("wo",), wo_s.at[1 - c])
        finish(stage, 1 - c, h)
        finish(seen, c, h)
        start(("seen", h), stage(c, h), seen(c, h), partner)
        if h == order[-1]:
            project(h, [c], False, False)
            arrived(("seen", h), seen(1 - c, h))
            project(h, [1 - c], False, True)
        else:
            arrived(("seen", h), seen(1 - c, h))
            project(h, [c, 1 - c], h == order[0], False)
    lax.fori_loop(0, 4, lambda i, _: out_copy(i).wait(), None)

    wo_copy.wait_send()
    for t in sent[settled:]:
        t.wait_send()
    left(range(3, far + 1))


def solution(mesh):
    chips = mesh.shape["sp"] // 2
    side = math.isqrt(mesh.shape["dp"])

    def step(x, gain, wq, wk, wv, wo):
        own, width = x.shape
        tokens = 2 * own
        half = HEAD // 2
        freq = jnp.asarray(THETA ** (-np.arange(half, dtype=np.float32) / half), jnp.float32).reshape(1, half)
        kvh = wk.shape[1] // HEAD // 2
        per = wq.shape[1] // wk.shape[1]
        far = chips // 2
        vm, hbm = pl.BlockSpec(memory_space=pltpu.VMEM), pl.BlockSpec(memory_space=pl.ANY)
        deep = wo.shape[0] * 2 * chips
        came = 5 * (4 * far + 1) + 5 + 1 + 3
        hops = 2 * (tokens // BK) * kvh
        return pl.pallas_call(
            functools.partial(_kernel, chips, side),
            out_shape=jax.ShapeDtypeStruct((own, width), jnp.bfloat16),
            in_specs=[hbm] + [vm] * 2 + [hbm] * 4,
            out_specs=hbm,
            scratch_shapes=[
                pltpu.VMEM((tokens, width), jnp.bfloat16),
                pltpu.VMEM((width, wk.shape[1] // 2), jnp.bfloat16),
                pltpu.VMEM((width, wv.shape[1] // 2), jnp.bfloat16),
                pltpu.VMEM((width, wq.shape[1] // 4), jnp.bfloat16),
                pltpu.VMEM((width, wq.shape[1] // 4), jnp.bfloat16),
                pltpu.VMEM((2, deep, width // 2), jnp.bfloat16),
                pltpu.VMEM((chips, kvh, tokens, HEAD), jnp.bfloat16),
                pltpu.VMEM((chips, kvh, HEAD, tokens), jnp.bfloat16),
                pltpu.VMEM((kvh, per * tokens, HEAD), jnp.bfloat16),
                pltpu.VMEM((kvh, 1, per * tokens), jnp.float32),
                pltpu.VMEM((kvh, HEAD + 8, per * tokens), jnp.float32),
                pltpu.VMEM((tokens, half), jnp.float32),
                pltpu.VMEM((tokens, half), jnp.float32),
                pltpu.VMEM((own, width), jnp.float32),
                pltpu.SemaphoreType.DMA((5 + 5 + 1 + 3,)),
                pltpu.SemaphoreType.DMA((came,)),
                pltpu.SemaphoreType.DMA((far * hops,)),
                pltpu.SemaphoreType.DMA(((far + 1) * hops,)),
                pltpu.SemaphoreType.DMA((6,)),
                pltpu.SemaphoreType.DMA((4,)),
            ],
            compiler_params=pltpu.CompilerParams(collective_id=0, has_side_effects=True, vmem_limit_bytes=VMEM),
            name="layer",
        )(x, gain, freq, wq, wk, wv, wo)

    tokens, whole = P(("dp", "sp"), None), P("sp", None)
    return jax.shard_map(
        step,
        mesh=mesh,
        in_specs=(tokens, P(None), whole, whole, whole, whole),
        out_specs=tokens,
        check_vma=False,
    )
```
